32 devices in a mesh: seq: 4 (over x, core), tp: 8 (over z, y).
Axes of the slice: x: 2, y: 2, z: 4, core: 2. Of those that a mesh axis runs over, the one named last changes fastest.
Arguments:
- vit_input: bfloat16 [2048, 1280], P(('seq', 'tp')), may hold values from -6 to 6
- image_lengths: int32 [4, 2], P('seq'), may hold values from 1 to 96, 128 in all within a row
- positions: int32 [512], replicated, may hold values from 0 to 511, each once
- vit_ln_gain: float32 [1280], replicated, may hold values from 0.25 to 1.75
- w_qkv: bfloat16 [1280, 3, 1280], P(None, None, 'tp'), may hold values from -0.15625 to 0.15625
- w_proj: bfloat16 [1280, 1280], P('tp'), may hold values from -0.15625 to 0.15625
- merger_ln_gain: float32 [1280], replicated, may hold values from 0.25 to 1.75
- merger_w1: bfloat16 [5120, 5120], P(None, 'tp'), may hold values from -0.078125 to 0.078125
- merger_w2: bfloat16 [5120, 8192], P('tp'), may hold values from -0.36336105 to 0.36336105
- norm_gain: float32 [8192], P('seq'), may hold values from 0.25 to 1.75
- gate_up_weight: bfloat16 [8192, 2, 29568], P('seq', None, 'tp'), may hold values from -0.0625 to 0.0625
- down_weight: bfloat16 [29568, 8192], P('tp', 'seq'), may hold values from -0.125 to 0.125
Outputs:
- mixed: bfloat16 [512, 8192], P('tp', 'seq')
The draws below stay inside these ranges and needn't reach their ends.
Inputs may be any that keep to these rules, and one draw needn't show every extreme that they name: `image_lengths`: each row sums to 128. `positions`: a permutation: every slot once.
All inputs are finite; a program needn't handle non-finite values.
Results may differ from the reference program's by a relative error of at most 0.038.
Values may be sent and summed in bfloat16 or wider, within the bound.
A program may use at most 128 MiB of HBM per device.

```python
import math
import jax
import jax.numpy as jnp
import numpy as np
from jax import lax

VW = 1280
HEADS = 16
D = 8192
FF = 29568
IMG_GROUP = 2
HD = 80
MW = 5120
GROUPS = 4
GROUP_TOK = 128
TOKENS = 512
PATCHES = 2048
N_SEQ = 4
N_TP = 8


def draw_merger_w2(key, part):
    first = jax.random.fold_in(key, 11)
    second = jax.random.fold_in(key, 23)
    third = jax.random.fold_in(key, 37)
    base = jnp.clip(jax.random.normal(first, (MW, D), jnp.float32), -6.0, 6.0)
    column_place = jnp.arange(D, dtype=jnp.float32) / D
    rough = jnp.exp(jax.random.uniform(second, (D,), jnp.float32, jnp.log(0.7), jnp.log(1.4)))
    column_scale = jnp.exp(jnp.log(3.0) * column_place) * rough
    pairing = jax.random.permutation(third, N_TP)
    row_block = jnp.arange(MW, dtype=jnp.int32) // (MW // N_TP)
    col_block = jnp.arange(D, dtype=jnp.int32) // (D // N_TP)
    spiked = pairing[row_block][:, None] == col_block[None, :]
    boost = jnp.where(spiked, 4.0, 1.0)
    values = base * boost * column_scale[None, :] / jnp.sqrt(16.0 * MW)
    return values.astype(jnp.bfloat16)


def levels(key, extent, shards, smallest, high):
    factor_of = 1.0
    for axis_at, blocks in shards:
        steps = jax.random.uniform(jax.random.fold_in(jax.random.fold_in(key, 6), axis_at), (blocks,), jnp.float32, smallest / len(shards), high / len(shards))
        factor_of = factor_of * jnp.repeat(jnp.exp(steps), extent[axis_at] // blocks).reshape((-1,) + (1,) * (len(extent) - 1 - axis_at))
    return factor_of


def length_profile(number_of, total, limit, slope):
    portions = [(1 << 20) // math.isqrt(standing ** slope) + 1 for standing in range(2, number_of + 1)]
    spare, holding = total - limit - (number_of - 1), [1] * (number_of - 1)
    while spare > 0:
        free = [i for i in range(number_of - 1) if holding[i] < limit]
        pool, remaining = sum([portions[i] for i in free]), spare
        for i in free:
            more = min(limit - holding[i], max(1, remaining * portions[i] // pool), spare)
            holding[i] = holding[i] + more
            spare = spare - more
    return np.array([limit] + holding)


def uneven(stream_key, number_of, total, limit, lean):
    if number_of == 2:
        one = jax.random.randint(stream_key, (), max(1, total - limit), min(limit, total - 1) + 1)
        return jnp.stack([one, total - one])
    tallies = jnp.asarray(length_profile(number_of, total, limit, lean), jnp.int32)
    twos = (number_of - 1) // 2
    source_of, receiver = tallies[1:1 + 2 * twos:2], tallies[2:2 + 2 * twos:2]
    slack = jnp.minimum(source_of - 1, limit - receiver)
    moved = jax.random.randint(jax.random.fold_in(stream_key, 1), (twos,), 0, 1 << 20) % (slack + 1)
    tallies = tallies.at[1:1 + 2 * twos:2].set(source_of - moved).at[2:2 + 2 * twos:2].set(receiver + moved)
    return tallies[jax.random.permutation(jax.random.fold_in(stream_key, 2), number_of)]


def bell_draw(rng, dims, scale, reach, pieces=(), kind=jnp.bfloat16):
    factor_of = levels(rng, dims, pieces, -0.22, 0.18) if pieces else 1.0
    entries = jax.random.normal(rng, dims, jnp.float32) * scale * factor_of
    return jnp.minimum(jnp.maximum(entries, -reach), reach).astype(kind)


def setup_inputs(seed: int = 0) -> dict:
    streams_of = jax.random.split(jax.random.key(seed), 13)
    return {
        "vit_input": bell_draw(streams_of[0], (PATCHES, VW), 1.0, 6.0, ((0, 32),)),
        "image_lengths": jax.vmap(lambda own: uneven(own, IMG_GROUP, GROUP_TOK, GROUP_TOK * 3 // 4, 2))(jax.random.split(streams_of[1], GROUPS)).reshape((GROUPS, IMG_GROUP)).astype(jnp.int32),
        "positions": jax.random.permutation(streams_of[2], TOKENS).astype(jnp.int32),
        "vit_ln_gain": jnp.clip(1.0 + 0.15 * jax.random.normal(streams_of[3], (VW,), jnp.float32), 0.25, 1.75),
        "w_qkv": bell_draw(streams_of[4], (VW, 3, VW), VW ** -0.5, 0.15625, ((2, 8),)),
        "w_proj": bell_draw(streams_of[5], (VW, VW), VW ** -0.5, 0.15625, ((0, 8),)),
        "merger_ln_gain": jnp.clip(1.0 + 0.15 * jax.random.normal(streams_of[6], (VW,), jnp.float32), 0.25, 1.75),
        "merger_w1": bell_draw(streams_of[7], (MW, MW), MW ** -0.5, 0.078125, ((1, 8),)),
        "merger_w2": draw_merger_w2(jax.random.fold_in(streams_of[12], 71), 0),
        "norm_gain": jnp.clip(1.0 + 0.15 * jax.random.normal(streams_of[9], (D,), jnp.float32), 0.25, 1.75),
        "gate_up_weight": bell_draw(streams_of[10], (D, 2, FF), D ** -0.5, 0.0625, ((0, 4), (2, 8))),
        "down_weight": bell_draw(streams_of[11], (FF, D), (FF // 16) ** -0.5, 0.125, ((0, 8), (1, 4))),
    }


def layer_norm(values, gain):
    mean = lax.optimization_barrier(jnp.mean(values, axis=-1, keepdims=True))
    centered = values - mean
    variance = lax.optimization_barrier(jnp.mean(centered * centered, axis=-1, keepdims=True))
    return centered * lax.rsqrt(variance + 1e-06) * gain

def image_ids(lengths, count):
    image_ends = jnp.cumsum(lengths.astype(jnp.int32)) * 4
    patch_index = jnp.arange(count, dtype=jnp.int32)
    return lax.optimization_barrier(jnp.sum((patch_index[:, None] >= image_ends[None, :]).astype(jnp.int32), axis=1))

def wire_round(values):
    return lax.optimization_barrier(values.astype(jnp.bfloat16)).astype(jnp.float32)

def attend(query, keys, values, image_index):
    scores = jnp.einsum('qhe,khe->hqk', query.astype(jnp.float32), keys.astype(jnp.float32)) * HD ** (-0.5)
    same_image = image_index[:, None] == image_index[None, :]
    scores = jnp.where(same_image[None], scores, -1e+30)
    top = lax.optimization_barrier(jnp.max(scores, axis=-1, keepdims=True))
    expo = jnp.exp(scores - top)
    weights = (expo / lax.optimization_barrier(jnp.sum(expo, axis=-1, keepdims=True))).astype(jnp.bfloat16)
    output = jnp.einsum('hqk,khe->qhe', weights.astype(jnp.float32), values.astype(jnp.float32))
    return output.astype(jnp.bfloat16)

def slot_sources(positions):
    count = positions.shape[0]
    return jnp.zeros((count,), jnp.int32).at[positions.astype(jnp.int32)].set(jnp.arange(count, dtype=jnp.int32))

def reference(vit_input, image_lengths, positions, vit_ln_gain, w_qkv, w_proj, merger_ln_gain, merger_w1, merger_w2, norm_gain, gate_up_weight, down_weight):
    group_patches = PATCHES // N_SEQ
    normed_patches = layer_norm(vit_input.astype(jnp.float32), vit_ln_gain).astype(jnp.bfloat16)
    projected = jnp.dot(normed_patches, w_qkv.reshape(VW, 3 * VW), preferred_element_type=jnp.float32).astype(jnp.bfloat16)
    projected = projected.reshape(N_SEQ, group_patches, 3, HEADS, HD)

    def per_group(pair):
        block, lengths = pair
        image_index = image_ids(lengths, group_patches)
        return attend(block[:, 0], block[:, 1], block[:, 2], image_index)
    attended = lax.map(per_group, (projected, image_lengths)).reshape(PATCHES, VW)
    head_cols = VW // N_TP
    attn_sum = jnp.zeros((PATCHES, VW), jnp.float32)
    for block_index in range(N_TP):
        lower = block_index * head_cols
        attn_sum = attn_sum + wire_round(jnp.dot(attended[:, lower:lower + head_cols], w_proj[lower:lower + head_cols], preferred_element_type=jnp.float32))
    vit_out = vit_input.astype(jnp.float32) + attn_sum
    merged_in = layer_norm(vit_out, merger_ln_gain).astype(jnp.bfloat16).reshape(TOKENS, MW)
    expanded = jax.nn.gelu(jnp.dot(merged_in, merger_w1, preferred_element_type=jnp.float32), approximate=False).astype(jnp.bfloat16)
    merge_cols = MW // N_TP
    vis_sum = jnp.zeros((TOKENS, D), jnp.float32)
    for block_index in range(N_TP):
        lower = block_index * merge_cols
        vis_sum = vis_sum + wire_round(jnp.dot(expanded[:, lower:lower + merge_cols], merger_w2[lower:lower + merge_cols], preferred_element_type=jnp.float32))
    vis = vis_sum.astype(jnp.bfloat16)
    seq_tokens = jnp.take(vis, slot_sources(positions), axis=0)
    token_values = seq_tokens.astype(jnp.float32)
    row_squares = lax.optimization_barrier(jnp.sum(token_values * token_values, axis=1))
    inverse_rms = lax.rsqrt(row_squares / D + 1e-06)
    normed = (token_values * inverse_rms[:, None] * norm_gain).astype(jnp.bfloat16)
    slice_width = D // N_SEQ
    gate_up = jnp.zeros((TOKENS, 2 * FF), jnp.float32)
    for block_index in range(N_SEQ):
        lower = block_index * slice_width
        weight_block = gate_up_weight[lower:lower + slice_width].reshape(slice_width, 2 * FF)
        gate_up = gate_up + wire_round(jnp.dot(normed[:, lower:lower + slice_width], weight_block, preferred_element_type=jnp.float32))
    hidden = (jax.nn.silu(gate_up[:, :FF]) * gate_up[:, FF:]).astype(jnp.bfloat16)
    hidden_cols = FF // N_TP
    down_sum = jnp.zeros((TOKENS, D), jnp.float32)
    for block_index in range(N_TP):
        lower = block_index * hidden_cols
        down_sum = down_sum + wire_round(jnp.dot(hidden[:, lower:lower + hidden_cols], down_weight[lower:lower + hidden_cols], preferred_element_type=jnp.float32))
    return (token_values + down_sum).astype(jnp.bfloat16)
```

```python
import functools

import jax
import jax.numpy as jnp
from jax import lax
from jax.experimental import pallas as pl
from jax.experimental.pallas import tpu as pltpu
from jax.sharding import PartitionSpec as P

HD = 80
MESH = pl.DeviceIdType.MESH
VM = pl.BlockSpec(memory_space=pltpu.VMEM)


def factors(n):
    minor = max(d for d in range(1, n + 1) if n % d == 0 and d * d <= n)
    return n // minor, minor


def greet(axis, peers):
    barrier = pltpu.get_barrier_semaphore()
    for peer in peers:
        pl.semaphore_signal(barrier, inc=1, device_id={axis: peer}, device_id_type=MESH)
    pl.semaphore_wait(barrier, len(peers))


def grid_peers(n_a, n_b, a, b):
    along_a = [lax.rem(a + da, n_a) * n_b + b for da in range(1, n_a)]
    along_b = [a * n_b + lax.rem(b + db, n_b) for db in range(1, n_b)]
    return along_a, along_b


def remote(src, dst, send_sem, recv_sem, axis, peer):
    return pltpu.make_async_remote_copy(
        src_ref=src,
        dst_ref=dst,
        send_sem=send_sem,
        recv_sem=recv_sem,
        device_id={axis: peer},
        device_id_type=MESH,
    )


def send(*args):
    copy = remote(*args)
    copy.start()
    return copy


def gather_kernel(axis, n, x_ref, out_ref, a_send, a_recv, b_send, b_recv, own_sem):
    n_a, n_b = factors(n)
    me = lax.axis_index(axis)
    a, b = me // n_b, lax.rem(me, n_b)
    along_a, along_b = grid_peers(n_a, n_b, a, b)
    greet(axis, along_a + along_b)
    a_copies, b_copies = [None], []
    for da in range(1, n_a):
        a_copies.append(
            send(x_ref, out_ref.at[me], a_send.at[da - 1], a_recv.at[da - 1], axis, along_a[da - 1])
        )
    own = pltpu.make_async_copy(x_ref, out_ref.at[me], own_sem)
    own.start()
    for db in range(1, n_b):
        b_copies.append(
            send(x_ref, out_ref.at[me], b_send.at[0, db - 1], b_recv.at[0, db - 1], axis, along_b[db - 1])
        )
    order = sorted(range(1, n_a), key=lambda da: min(da, n_a - da))
    for da in order:
        a_copies[da].wait_recv()
        source = lax.rem(a - da + n_a, n_a) * n_b + b
        for db in range(1, n_b):
            b_copies.append(
                send(
                    out_ref.at[source],
                    out_ref.at[source],
                    b_send.at[da, db - 1],
                    b_recv.at[da, db - 1],
                    axis,
                    along_b[db - 1],
                )
            )
    for copy in b_copies:
        copy.wait()
    for copy in a_copies[1:]:
        copy.wait_send()
    own.wait()


def gather(x, axis, collective_id):
    n = lax.axis_size(axis)
    n_a, n_b = factors(n)
    dma = pltpu.SemaphoreType.DMA
    return pl.pallas_call(
        functools.partial(gather_kernel, axis, n),
        out_shape=jax.ShapeDtypeStruct((n,) + x.shape, x.dtype),
        in_specs=[VM],
        out_specs=VM,
        scratch_shapes=[
            dma((n_a,)),
            dma((n_a,)),
            dma((n_a, n_b)),
            dma((n_a, n_b)),
            dma,
        ],
        name=f"gather{collective_id}",
        compiler_params=pltpu.CompilerParams(collective_id=collective_id, has_side_effects=True),
    )(x)


def scatter_kernel(axis, n, x_ref, out_ref, r1, y, r2, a_send, a_recv, b_send, b_recv):
    n_a, n_b = factors(n)
    me = lax.axis_index(axis)
    a, b = me // n_b, lax.rem(me, n_b)
    along_a, along_b = grid_peers(n_a, n_b, a, b)
    greet(axis, along_a + along_b)
    order = sorted(range(1, n_a), key=lambda da: -min(da, n_a - da)) + [0]
    b_copies, a_copies = {}, []
    for da in order:
        for db in range(1, n_b):
            block = lax.rem(a + da, n_a) * n_b + lax.rem(b + db, n_b)
            b_copies[da, db] = send(
                x_ref.at[block],
                r1.at[da, db - 1],
                b_send.at[da, db - 1],
                b_recv.at[da, db - 1],
                axis,
                along_b[db - 1],
            )

    def arrived(da):
        total = x_ref[lax.rem(a + da, n_a) * n_b + b].astype(jnp.float32)
        for db in range(1, n_b):
            b_copies[da, db].wait_recv()
            total = total + r1[da, db - 1].astype(jnp.float32)
        return total

    for da in order[:-1]:
        y[da - 1] = arrived(da).astype(y.dtype)
        a_copies.append(
            send(y.at[da - 1], r2.at[da - 1], a_send.at[da - 1], a_recv.at[da - 1], axis, along_a[da - 1])
        )
    total = arrived(0)
    for da, copy in zip(order[:-1], a_copies):
        copy.wait_recv()
        total = total + r2[da - 1].astype(jnp.float32)
    out_ref[...] = total.astype(out_ref.dtype)
    for copy in b_copies.values():
        copy.wait_send()
    for copy in a_copies:
        copy.wait_send()


def scatter_sum(x, axis, dtype, collective_id):
    n = lax.axis_size(axis)
    n_a, n_b = factors(n)
    block = x.shape[1:]
    dma = pltpu.SemaphoreType.DMA
    return pl.pallas_call(
        functools.partial(scatter_kernel, axis, n),
        out_shape=jax.ShapeDtypeStruct(block, dtype),
        in_specs=[VM],
        out_specs=VM,
        scratch_shapes=[
            pltpu.VMEM((n_a, n_b - 1) + block, x.dtype),
            pltpu.VMEM((n_a - 1,) + block, x.dtype),
            pltpu.VMEM((n_a - 1,) + block, x.dtype),
            dma((n_a,)),
            dma((n_a,)),
            dma((n_a, n_b)),
            dma((n_a, n_b)),
        ],
        name=f"scatter_sum{collective_id}",
        compiler_params=pltpu.CompilerParams(collective_id=collective_id, has_side_effects=True),
    )(x)


SEMS = (
    "w2", "w", "d", "ea_s", "ea_r", "eb_s", "eb_r", "q_s", "q_r", "p_s", "p_r", "y_s", "y_r", "h_s", "h_r",
    "o_s", "b_r", "rb_s", "rb_r", "ra_s", "ra_r", "ga_s", "ga_r", "gb_s", "gb_r",
)
BUFS = (
    "ex", "w2s", "part", "r1", "yb", "r2", "tok", "nrm", "sqa", "rq", "inv", "held", "dheld", "gu", "pin",
    "keep", "yx", "rx", "hid", "acc",
)


def decoder_kernel(parts, e_ref, pos_ref, gain_ref, w2_ref, w_ref, d_ref, out_ref, *scratch):
    buf = dict(zip(BUFS, scratch))
    sem = dict(zip(SEMS, scratch[len(BUFS):]))
    n, m = lax.axis_size("seq"), lax.axis_size("tp")
    (n_a, n_b), (m_a, m_b) = factors(n), factors(m)
    me, mt = lax.axis_index("seq"), lax.axis_index("tp")
    a, b = me // n_b, lax.rem(me, n_b)
    ta, tb = mt // m_b, lax.rem(mt, m_b)
    x_peers, core_peers = grid_peers(n_a, n_b, a, b)
    t_major, t_minor = grid_peers(m_a, m_b, ta, tb)
    partner = core_peers[0]
    chunks, rows, depth = w_ref.shape[1:]
    steps = parts * chunks
    owned = steps // n_b
    count = n_a * 128
    block = count // m

    def to(axis, src, dst, s, r, peer):
        return remote(src, dst, s, r, axis, peer)

    def lanes(owner):
        return pl.ds(pl.multiple_of(owner * 128, 128), 128)

    w2_load = pltpu.make_async_copy(
        w2_ref.at[:, pl.ds(pl.multiple_of(me * depth, depth), depth)], buf["w2s"], sem["w2"]
    )

    def w_load(i):
        slot = lax.rem(i, 2)
        return pltpu.make_async_copy(w_ref.at[:, lax.rem(i, chunks)], buf["held"].at[slot], sem["w"].at[slot])

    def d_load(i):
        slot = lax.rem(i, 2)
        return pltpu.make_async_copy(d_ref.at[lax.rem(i, chunks)], buf["dheld"].at[slot], sem["d"].at[slot])

    w2_load.start()
    w_load(0).start()

    barrier = pltpu.get_barrier_semaphore()
    everyone = [("seq", lax.rem(me + d, n)) for d in range(1, n)]
    everyone += [("tp", peer) for peer in t_major + t_minor]
    for axis, peer in everyone:
        pl.semaphore_signal(barrier, inc=1, device_id={axis: peer}, device_id_type=MESH)
    pl.semaphore_wait(barrier, len(everyone))

    ex = buf["ex"]
    e_a = [
        to("seq", e_ref, ex.at[me], sem["ea_s"].at[da - 1], sem["ea_r"].at[da - 1], x_peers[da - 1])
        for da in range(1, n_a)
    ]
    e_b = [to("seq", e_ref, ex.at[me], sem["eb_s"].at[0], sem["eb_r"].at[0], partner)]
    for copy in e_a + e_b:
        copy.start()
    ex[me] = e_ref[...]
    for da in range(1, n_a):
        e_a[da - 1].wait_recv()
        source = ex.at[lax.rem(a - da + n_a, n_a) * n_b + b]
        copy = to("seq", source, source, sem["eb_s"].at[da], sem["eb_r"].at[da], partner)
        copy.start()
        e_b.append(copy)
    for copy in e_b:
        copy.wait()
    for copy in e_a:
        copy.wait_send()

    part, r1, yb, r2 = buf["part"], buf["r1"], buf["yb"], buf["r2"]
    order = sorted(range(1, m_a), key=lambda da: -min(da, m_a - da)) + [0]

    def rs_minor(u, da, db):
        at = lax.rem(ta + da, m_a) * m_b + lax.rem(tb + db, m_b)
        return to(
            "tp", part.at[u, at], r1.at[u, da, db - 1], sem["rb_s"].at[u, da, db - 1],
            sem["rb_r"].at[u, da, db - 1], t_minor[db - 1],
        )

    def rs_major(u, da):
        return to(
            "tp", yb.at[u, da - 1], r2.at[u, da - 1], sem["ra_s"].at[u, da - 1], sem["ra_r"].at[u, da - 1],
            t_major[da - 1],
        )

    def rs_start(u):
        for da in order:
            for db in range(1, m_b):
                rs_minor(u, da, db).start()

    def rs_arrived(u, da):
        total = part[u, lax.rem(ta + da, m_a) * m_b + tb].astype(jnp.float32)
        for db in range(1, m_b):
            rs_minor(u, da, db).wait_recv()
            total = total + r1[u, da, db - 1].astype(jnp.float32)
        return total

    def rs_pass(u):
        for da in order[:-1]:
            yb[u, da - 1] = rs_arrived(u, da).astype(yb.dtype)
            rs_major(u, da).start()

    def rs_finish(u):
        total = rs_arrived(u, 0)
        for da in order[:-1]:
            rs_major(u, da).wait_recv()
            total = total + r2[u, da - 1].astype(jnp.float32)
        for da in order:
            for db in range(1, m_b):
                rs_minor(u, da, db).wait_send()
        for da in order[:-1]:
            rs_major(u, da).wait_send()
        return total

    tok = buf["tok"]

    def ag_major(h, da):
        return to(
            "tp", tok.at[h, mt], tok.at[h, mt], sem["ga_s"].at[h, da - 1], sem["ga_r"].at[h, da - 1], t_major[da - 1]
        )

    def ag_minor(h, da, db):
        at = lax.rem(ta - da + m_a, m_a) * m_b + tb
        return to(
            "tp", tok.at[h, at], tok.at[h, at], sem["gb_s"].at[h, da, db - 1], sem["gb_r"].at[h, da, db - 1],
            t_minor[db - 1],
        )

    near = order[:-1][::-1]

    def ag_start(h):
        tok[h, mt] = rs_finish(h).astype(tok.dtype)
        for da in order[:-1]:
            ag_major(h, da).start()
        for db in range(1, m_b):
            ag_minor(h, 0, db).start()

    def ag_relay(h):
        for da in near:
            ag_major(h, da).wait_recv()
            for db in range(1, m_b):
                ag_minor(h, da, db).start()

    rq, inv, sqa, nrm = buf["rq"], buf["inv"], buf["sqa"], buf["nrm"]

    def squares(h, d):
        return to(
            "seq", rq.at[h, me], rq.at[h, me], sem["q_s"].at[h, d - 1], sem["q_r"].at[h, d - 1], lax.rem(me + d, n)
        )

    def ag_finish(h):
        for da in [0] + near:
            for db in range(1, m_b):
                ag_minor(h, da, db).wait()
        for da in near:
            ag_major(h, da).wait_send()

        def rows_of(t, carry):
            values = tok[h, t].astype(jnp.float32)
            at = pl.ds(pl.multiple_of(t * block, block), block)
            nrm[at] = (values * gain_ref[...]).astype(nrm.dtype)
            total = values[:, :128] * values[:, :128]
            for k in range(1, depth // 128):
                piece = values[:, k * 128 : (k + 1) * 128]
                total = total + piece * piece
            sqa[at] = total
            return carry

        lax.fori_loop(0, m, rows_of, 0)
        sums = jnp.sum(jnp.transpose(sqa[...]), axis=0, keepdims=True)
        rq[h, me] = jnp.broadcast_to(sums, (8, count))
        for d in range(1, n):
            squares(h, d).start()

    def inverse(h):
        for d in range(1, n):
            squares(h, d).wait()
        total = rq[h, 0]
        for s in range(1, n):
            total = total + rq[h, s]
        inv[h] = lax.rsqrt(total / (depth * n) + 1e-06)

    w2_load.wait()
    for h in range(parts):
        row = lax.broadcasted_iota(jnp.int32, (count, pos_ref.shape[1]), 0)
        slot = lax.shift_right_logical(row, block.bit_length() - 1) * (block * (parts - 1)) + row + h * block
        pick = (slot == pos_ref[...]).astype(jnp.bfloat16)
        moved = jnp.dot(
            pick, ex[...].reshape(pos_ref.shape[1], ex.shape[2]), preferred_element_type=jnp.float32
        ).astype(jnp.bfloat16)
        width = min(512, depth)
        for k in range(depth // width):
            piece = jnp.dot(
                moved, buf["w2s"][:, k * width : (k + 1) * width], preferred_element_type=jnp.float32
            ).astype(part.dtype)
            part[h, :, :, k * width : (k + 1) * width] = piece.reshape(m, block, width)
        if h == 0:
            rs_start(0)
    rs_pass(0)
    ag_start(0)
    ag_relay(0)
    ag_finish(0)

    gu, pin, keep, yx, rx, hid, acc = (buf[k] for k in ("gu", "pin", "keep", "yx", "rx", "hid", "acc"))

    def owner(i):
        return lax.rem(i, n_b) == b

    def to_owner(i):
        return to("seq", gu.at[lax.rem(i, 2)], pin.at[i // n_b], sem["p_s"].at[i // n_b], sem["p_r"].at[i // n_b], partner)

    def to_x(i, da):
        o = i // n_b
        return to(
            "seq", yx.at[o, da - 1], rx.at[o, da - 1], sem["y_s"].at[o, da - 1], sem["y_r"].at[o, da - 1], x_peers[da - 1]
        )

    def hid_x(i, da):
        target = hid.at[i, :, lanes(a)]
        return to("seq", target, target, sem["h_s"].at[i, da - 1], sem["h_r"].at[i, da - 1], x_peers[da - 1])

    def hid_core(i, da):
        target = hid.at[i, :, lanes(lax.rem(a - da + n_a, n_a))]
        return to("seq", target, target, sem["o_s"].at[i, da], sem["b_r"].at[i, da], partner)

    def stage_a(i):
        w_load(i).wait()

        @pl.when(i + 1 < steps)
        def _():
            w_load(i + 1).start()

        for half in range(2):
            gu[lax.rem(i, 2), half] = lax.dot_general(
                buf["held"][lax.rem(i, 2), half],
                nrm[...],
                (((1,), (1,)), ((), ())),
                preferred_element_type=jnp.float32,
            ).astype(gu.dtype)

        @pl.when(jnp.logical_not(owner(i)))
        def _():
            to_owner(i).start()

    def stage_b(i):
        o = i // n_b

        @pl.when(owner(i))
        def _():
            to_owner(i).wait_recv()

            def both(da):
                at = lanes(lax.rem(a + da, n_a))
                return gu[lax.rem(i, 2), :, :, at].astype(jnp.float32) + pin[o, :, :, at].astype(jnp.float32)

            for da in range(1, n_a):
                yx[o, da - 1] = both(da).astype(yx.dtype)
                to_x(i, da).start()
            keep[lax.rem(o, 2)] = both(0)

        @pl.when(jnp.logical_not(owner(i)))
        def _():
            to_owner(i).wait_send()

    def stage_c(i):
        o, h = i // n_b, i // chunks

        @pl.when(lax.rem(i, chunks) == 0)
        def _():
            inverse(h)

        @pl.when(owner(i))
        def _():
            total = keep[lax.rem(o, 2)]
            for da in range(1, n_a):
                to_x(i, da).wait()
                total = total + rx[o, da - 1].astype(jnp.float32)
            total = total * inv[h, 0:1, lanes(a)]
            hid[i, :, lanes(a)] = (jax.nn.silu(total[0]) * total[1]).astype(hid.dtype)
            for da in range(1, n_a):
                hid_x(i, da).start()
            hid_core(i, 0).start()

    def stage_d(i):
        @pl.when(owner(i))
        def _():
            for da in range(1, n_a):
                hid_x(i, da).wait()
                hid_core(i, da).start()

    def stage_e(i):
        c, h = lax.rem(i, chunks), i // chunks

        @pl.when(owner(i))
        def _():
            for da in range(n_a):
                hid_core(i, da).wait_send()

        @pl.when(jnp.logical_not(owner(i)))
        def _():
            for da in range(n_a):
                hid_core(i, da).wait_recv()

        d_load(i).wait()
        width = min(512, depth)
        left = hid[i]
        for k in range(depth // width):
            at = slice(k * width, (k + 1) * width)
            piece = lax.dot_general(
                left, buf["dheld"][lax.rem(i, 2), :, at], (((0,), (0,)), ((), ())), preferred_element_type=jnp.float32
            )

            @pl.when(c == 0)
            def _():
                acc[:, at] = piece

            @pl.when(c > 0)
            def _():
                acc[:, at] += piece

        @pl.when(c == chunks - 1)
        def _():
            part[parts + h] = acc[...].astype(part.dtype).reshape(m, block, depth)
            rs_start(parts + h)

    def output(h):
        at = pl.ds(pl.multiple_of(h * block, block), block)
        total = rs_finish(parts + h)
        out_ref[at] = (tok[h, mt].astype(jnp.float32) + total).astype(out_ref.dtype)

    k_pass, k_gather, k_relay = 2 * chunks // 7, 4 * chunks // 7, 6 * chunks // 7

    def iteration(i, carry):
        def when(lag, fn):
            @pl.when(jnp.logical_and(i >= lag, i - lag < steps))
            def _():
                fn(i - lag)

        h, k = i // chunks, lax.rem(i, chunks)
        more = h + 1 < parts

        def at_step(step, fn):
            @pl.when(jnp.logical_and(more, k == step))
            def _():
                fn(h + 1)

        @pl.when(jnp.logical_and(jnp.logical_and(i > 0, i < steps), k == 0))
        def _():
            ag_finish(h)

        at_step(0, rs_start)
        when(3, lambda j: d_load(j).start())
        when(0, stage_a)
        when(1, stage_b)
        when(2, stage_c)
        when(3, stage_d)
        at_step(k_pass, rs_pass)
        at_step(k_gather, ag_start)
        at_step(k_relay, ag_relay)
        when(4, stage_e)

        def later(lag, fn):
            @pl.when(jnp.logical_and(i - lag >= chunks, jnp.logical_and(lax.rem(i - lag + chunks, chunks) == 0, i - lag < steps)))
            def _():
                fn((i - lag) // chunks - 1)

        later(5, lambda h: rs_pass(parts + h))
        later(7, output)
        return carry

    lax.fori_loop(0, steps + 4, iteration, 0)
    rs_pass(2 * parts - 1)
    output(parts - 1)


def decoder(expanded, positions, gain, w2, weight, down, collective_id):
    n, m = lax.axis_size("seq"), lax.axis_size("tp")
    (n_a, n_b), (m_a, m_b) = factors(n), factors(m)
    _, chunks, rows, depth = weight.shape
    tokens = positions.shape[1]
    count = n_a * 128
    parts = tokens // count
    steps = parts * chunks
    block = count // m
    assert n_b == 2 and steps % 2 == 0 and chunks >= 7
    kind, f32 = expanded.dtype, jnp.float32
    shapes = {
        "ex": ((n,) + expanded.shape, kind),
        "w2s": ((w2.shape[0], depth), kind),
        "part": ((2 * parts, m, block, depth), kind),
        "r1": ((2 * parts, m_a, m_b - 1, block, depth), kind),
        "yb": ((2 * parts, m_a - 1, block, depth), kind),
        "r2": ((2 * parts, m_a - 1, block, depth), kind),
        "tok": ((parts, m, block, depth), kind),
        "nrm": ((count, depth), kind),
        "sqa": ((count, 128), f32),
        "rq": ((parts, n, 8, count), f32),
        "inv": ((parts, 8, count), f32),
        "held": ((2, 2, rows, depth), kind),
        "dheld": ((2, rows, depth), kind),
        "gu": ((2, 2, rows, count), kind),
        "pin": ((steps // 2, 2, rows, count), kind),
        "keep": ((2, 2, rows, 128), f32),
        "yx": ((steps // 2, n_a - 1, 2, rows, 128), kind),
        "rx": ((steps // 2, n_a - 1, 2, rows, 128), kind),
        "hid": ((steps, rows, count), kind),
        "acc": ((count, depth), f32),
    }
    sems = {
        "w2": (),
        "w": (2,),
        "d": (2,),
        "ea_s": (n_a,),
        "ea_r": (n_a,),
        "eb_s": (n_a,),
        "eb_r": (n_a,),
        "q_s": (parts, n),
        "q_r": (parts, n),
        "p_s": (steps // 2,),
        "p_r": (steps // 2,),
        "y_s": (steps // 2, n_a),
        "y_r": (steps // 2, n_a),
        "h_s": (steps, n_a),
        "h_r": (steps, n_a),
        "o_s": (steps, n_a),
        "b_r": (steps, n_a),
        "rb_s": (2 * parts, m_a, m_b),
        "rb_r": (2 * parts, m_a, m_b),
        "ra_s": (2 * parts, m_a),
        "ra_r": (2 * parts, m_a),
        "ga_s": (parts, m_a),
        "ga_r": (parts, m_a),
        "gb_s": (parts, m_a, m_b),
        "gb_r": (parts, m_a, m_b),
    }
    anywhere = pl.BlockSpec(memory_space=pl.ANY)
    return pl.pallas_call(
        functools.partial(decoder_kernel, parts),
        out_shape=jax.ShapeDtypeStruct((tokens // m, depth), kind),
        in_specs=[VM, VM, VM, anywhere, anywhere, anywhere],
        out_specs=VM,
        scratch_shapes=[pltpu.VMEM(*shapes[k]) for k in BUFS]
        + [pltpu.SemaphoreType.DMA(sems[k]) if sems[k] else pltpu.SemaphoreType.DMA for k in SEMS],
        name="decoder",
        compiler_params=pltpu.CompilerParams(
            collective_id=collective_id, has_side_effects=True, vmem_limit_bytes=67_000_000
        ),
    )(expanded, positions, gain, w2, weight, down)


def chunk_count(rows):
    for count in (7, 6, 4, 3, 2):
        if rows % (count * 8) == 0:
            return count
    return 1


def layer_norm(values, gain):
    mean = jnp.mean(values, axis=-1, keepdims=True)
    centered = values - mean
    variance = jnp.mean(centered * centered, axis=-1, keepdims=True)
    return centered * lax.rsqrt(variance + 1e-06) * gain


def image_ids(lengths, count):
    image_ends = jnp.cumsum(lengths) * 4
    patch_index = jnp.arange(count, dtype=jnp.int32)
    return jnp.sum((patch_index[:, None] >= image_ends[None, :]).astype(jnp.int32), axis=1)


def attend(query, keys, values, image_index):
    scores = jnp.einsum("qhe,khe->hqk", query, keys, preferred_element_type=jnp.float32) * HD ** (
        -0.5
    )
    same_image = image_index[:, None] == image_index[None, :]
    scores = jnp.where(same_image[None], scores, -1e30)
    top = jnp.max(scores, axis=-1, keepdims=True)
    expo = jnp.exp(scores - top)
    weights = (expo / jnp.sum(expo, axis=-1, keepdims=True)).astype(jnp.bfloat16)
    output = jnp.einsum("hqk,khe->qhe", weights, values, preferred_element_type=jnp.float32)
    return output.astype(jnp.bfloat16)


def local(
    vit_input,
    image_lengths,
    positions,
    vit_ln_gain,
    w_qkv,
    w_proj,
    merger_ln_gain,
    merger_w1,
    merger_w2,
    norm_gain,
    gate_up_weight,
    down_weight,
):
    tp_size = lax.axis_size("tp")
    own_patches = vit_input.shape[0]
    patch_width = vit_input.shape[1]
    head_cols = w_qkv.shape[2]
    local_heads = head_cols // HD
    normed_patches = layer_norm(vit_input.astype(jnp.float32), vit_ln_gain).astype(jnp.bfloat16)
    w_qkv_flat = w_qkv.reshape(patch_width, 3 * head_cols)
    projected = jnp.dot(
        gather(normed_patches, "tp", 0).reshape(tp_size * own_patches, patch_width),
        w_qkv_flat,
        preferred_element_type=jnp.float32,
    ).astype(jnp.bfloat16)
    group_patches = projected.shape[0]
    projected = projected.reshape(group_patches, 3, local_heads, HD)
    image_index = image_ids(image_lengths[0], group_patches)
    attended = attend(projected[:, 0], projected[:, 1], projected[:, 2], image_index).reshape(
        group_patches, head_cols
    )
    attn_part = jnp.dot(attended, w_proj, preferred_element_type=jnp.float32).astype(jnp.bfloat16)
    attn_sum = scatter_sum(
        attn_part.reshape(tp_size, own_patches, patch_width), "tp", jnp.float32, 1
    )
    vit_out = vit_input.astype(jnp.float32) + attn_sum
    own_tokens = own_patches // 4
    merged_in = (
        layer_norm(vit_out, merger_ln_gain)
        .astype(jnp.bfloat16)
        .reshape(own_tokens, 4 * patch_width)
    )
    expanded = jax.nn.gelu(
        jnp.dot(
            gather(merged_in, "tp", 2).reshape(tp_size * own_tokens, 4 * patch_width),
            merger_w1,
            preferred_element_type=jnp.float32,
        ),
        approximate=False,
    ).astype(jnp.bfloat16)
    slice_width = norm_gain.shape[0]
    hidden_width = gate_up_weight.shape[2]
    chunks = chunk_count(hidden_width)
    weight_rows = gate_up_weight.transpose(1, 2, 0).reshape(
        2, chunks, hidden_width // chunks, slice_width
    )
    down_rows = down_weight.reshape(chunks, hidden_width // chunks, slice_width)
    return decoder(
        expanded, positions[None, :], norm_gain[None, :], merger_w2, weight_rows, down_rows, 3
    )


def solution(mesh):
    return jax.shard_map(
        local,
        mesh=mesh,
        in_specs=(
            P(("seq", "tp"), None),
            P("seq", None),
            P(),
            P(),
            P(None, None, "tp"),
            P("tp", None),
            P(),
            P(None, "tp"),
            P("tp", None),
            P("seq"),
            P("seq", None, "tp"),
            P("tp", "seq"),
        ),
        out_specs=P("tp", "seq"),
        check_vma=False,
    )
```

```python
import functools

import jax
import jax.numpy as jnp
from jax import lax
from jax.experimental import pallas as pl
from jax.experimental.pallas import tpu as pltpu
from jax.sharding import PartitionSpec as P

HD = 80
MESH = pl.DeviceIdType.MESH
LAG_C, LAG_D, LAG_E = 3, 5, 6
AT_PASS, AT_GATHER, AT_RELAY = (1, 2), (3, 3), (4, 5, 6)
VM = pl.BlockSpec(memory_space=pltpu.VMEM)


def factors(n):
    minor = max(d for d in range(1, n + 1) if n % d == 0 and d * d <= n)
    return n // minor, minor


def grid_peers(n_a, n_b, a, b):
    along_a = [lax.rem(a + da, n_a) * n_b + b for da in range(1, n_a)]
    along_b = [a * n_b + lax.rem(b + db, n_b) for db in range(1, n_b)]
    return along_a, along_b


def remote(src, dst, send_sem, recv_sem, axis, peer):
    return pltpu.make_async_remote_copy(
        src_ref=src,
        dst_ref=dst,
        send_sem=send_sem,
        recv_sem=recv_sem,
        device_id={axis: peer},
        device_id_type=MESH,
    )


class LineGather:
    def __init__(self, view, sems):
        n = lax.axis_size("tp")
        self.n_a, self.n_b = factors(n)
        me = lax.axis_index("tp")
        self.a, self.b = me // self.n_b, lax.rem(me, self.n_b)
        self.minors = grid_peers(self.n_a, self.n_b, self.a, self.b)[1]
        self.view, self.sems = view, sems

    def up(self, u, src):
        block = self.view(u, src * self.n_b + self.b)
        send, recv = self.sems["u_s"].at[u, src], self.sems["u_r"].at[u, src]
        return remote(block, block, send, recv, "tp", lax.rem(self.a + 1, self.n_a) * self.n_b + self.b)

    def down(self, u, src):
        block = self.view(u, src * self.n_b + self.b)
        send, recv = self.sems["d_s"].at[u, src], self.sems["d_r"].at[u, src]
        return remote(block, block, send, recv, "tp", lax.rem(self.a + self.n_a - 1, self.n_a) * self.n_b + self.b)

    def minor(self, u, src, db):
        block = self.view(u, src * self.n_b + self.b)
        send, recv = self.sems["m_s"].at[u, src, db - 1], self.sems["m_r"].at[u, src, db - 1]
        return remote(block, block, send, recv, "tp", self.minors[db - 1])

    def send(self, u, src, upward, downward):
        if upward:
            @pl.when(self.a < self.n_a - 1)
            def _():
                self.up(u, src).start()
        if downward:
            @pl.when(self.a > 0)
            def _():
                self.down(u, src).start()
        for db in range(1, self.n_b):
            self.minor(u, src, db).start()

    def start(self, u):
        self.send(u, self.a, True, True)

    def relay(self, u, k):
        @pl.when(self.a >= k)
        def _():
            self.up(u, self.a - k).wait_recv()
            self.send(u, self.a - k, True, False)

        @pl.when(self.a + k < self.n_a)
        def _():
            self.down(u, self.a + k).wait_recv()
            self.send(u, self.a + k, False, True)

    def finish(self, u):
        for src in range(self.n_a):
            for db in range(1, self.n_b):
                self.minor(u, src, db).wait()

            @pl.when(jnp.logical_and(src <= self.a, self.a < self.n_a - 1))
            def _():
                self.up(u, src).wait_send()

            @pl.when(jnp.logical_and(src >= self.a, self.a > 0))
            def _():
                self.down(u, src).wait_send()


def line_sems(units):
    m_a, m_b = factors(lax.axis_size("tp"))
    return {
        "u_s": (units, m_a), "u_r": (units, m_a), "d_s": (units, m_a), "d_r": (units, m_a),
        "m_s": (units, m_a, m_b), "m_r": (units, m_a, m_b),
    }


class ScatterSum:
    def __init__(self, part, r1, yb, r2, sems):
        m = lax.axis_size("tp")
        self.n_a, self.n_b = factors(m)
        me = lax.axis_index("tp")
        self.a, self.b = me // self.n_b, lax.rem(me, self.n_b)
        self.majors, self.minors = grid_peers(self.n_a, self.n_b, self.a, self.b)
        self.part, self.r1, self.yb, self.r2, self.sems = part, r1, yb, r2, sems
        self.order = sorted(range(1, self.n_a), key=lambda da: -min(da, self.n_a - da)) + [0]

    def minor(self, u, da, db):
        at = lax.rem(self.a + da, self.n_a) * self.n_b + lax.rem(self.b + db, self.n_b)
        send, recv = self.sems["rb_s"].at[u, da, db - 1], self.sems["rb_r"].at[u, da, db - 1]
        return remote(self.part.at[u, at], self.r1.at[u, da, db - 1], send, recv, "tp", self.minors[db - 1])

    def major(self, u, da):
        send, recv = self.sems["ra_s"].at[u, da - 1], self.sems["ra_r"].at[u, da - 1]
        return remote(self.yb.at[u, da - 1], self.r2.at[u, da - 1], send, recv, "tp", self.majors[da - 1])

    def start(self, u):
        for da in self.order:
            for db in range(1, self.n_b):
                self.minor(u, da, db).start()

    def arrived(self, u, da):
        total = self.part[u, lax.rem(self.a + da, self.n_a) * self.n_b + self.b].astype(jnp.float32)
        for db in range(1, self.n_b):
            self.minor(u, da, db).wait_recv()
            total = total + self.r1[u, da, db - 1].astype(jnp.float32)
        return total

    def forward(self, u):
        for da in self.order[:-1]:
            self.yb[u, da - 1] = self.arrived(u, da).astype(self.yb.dtype)
            self.major(u, da).start()

    def finish(self, u):
        total = self.arrived(u, 0)
        for da in self.order[:-1]:
            self.major(u, da).wait_recv()
            total = total + self.r2[u, da - 1].astype(jnp.float32)
        for da in self.order:
            for db in range(1, self.n_b):
                self.minor(u, da, db).wait_send()
        for da in self.order[:-1]:
            self.major(u, da).wait_send()
        return total


def scatter_sems(units):
    m_a, m_b = factors(lax.axis_size("tp"))
    return {"rb_s": (units, m_a, m_b), "rb_r": (units, m_a, m_b), "ra_s": (units, m_a), "ra_r": (units, m_a)}


def scatter_shapes(units, block, kind):
    m_a, m_b = factors(lax.axis_size("tp"))
    return {
        "part": ((units, m_a * m_b) + block, kind),
        "r1": ((units, m_a, m_b - 1) + block, kind),
        "yb": ((units, m_a - 1) + block, kind),
        "r2": ((units, m_a - 1) + block, kind),
    }


def normalize(values, gain):
    mean = jnp.mean(values, axis=-1, keepdims=True)
    centered = values - mean
    variance = jnp.mean(centered * centered, axis=-1, keepdims=True)
    return centered * lax.rsqrt(variance + 1e-06) * gain


V_BUFS = ("ag", "wq", "wp", "w1", "qkv", "att", "part", "r1", "yb", "r2", "vo", "vs", "ag2")
V_SEMS = ("wq", "wp", "w1", "u_s", "u_r", "d_s", "d_r", "m_s", "m_r", "rb_s", "rb_r", "ra_s", "ra_r")


def vision_kernel(vit_ref, len_ref, gain_ref, gain2_ref, wq_ref, wp_ref, w1_ref, out_ref, *scratch):
    buf = dict(zip(V_BUFS, scratch))
    sem = dict(zip(V_SEMS, scratch[len(V_BUFS):]))
    m = lax.axis_size("tp")
    m_a, m_b = factors(m)
    mt = lax.axis_index("tp")
    own, width = vit_ref.shape
    half = width // 2
    heads_wide = wp_ref.shape[0]
    f32, kind = jnp.float32, vit_ref.dtype
    loads = {
        k: pltpu.make_async_copy(ref, buf[k], sem[k]) for k, ref in (("wq", wq_ref), ("wp", wp_ref), ("w1", w1_ref))
    }
    for copy in loads.values():
        copy.start()
    majors, minors = grid_peers(m_a, m_b, mt // m_b, lax.rem(mt, m_b))
    barrier = pltpu.get_barrier_semaphore()
    for peer in majors + minors:
        pl.semaphore_signal(barrier, inc=1, device_id={"tp": peer}, device_id_type=MESH)

    ag, ag2, vo, part, qkv, att = (buf[k] for k in ("ag", "ag2", "vo", "part", "qkv", "att"))
    first = normalize(vit_ref[...].astype(f32), gain_ref[...]).astype(kind)
    for q in range(2):
        ag[q, mt] = first[:, q * half : (q + 1) * half]
    pl.semaphore_wait(barrier, len(majors) + len(minors))

    def unit_view(u, at):
        return ag.at[u, at]

    gather_one = LineGather(unit_view, sem)
    for u in range(2):
        gather_one.start(u)
    for k in range(1, m_a):
        for u in range(2):
            gather_one.relay(u, k)
    loads["wq"].wait()
    patches = m * own
    for u in range(2):
        gather_one.finish(u)
        piece = lax.dot_general(
            buf["wq"][:, u * half : (u + 1) * half],
            ag[u].reshape(patches, half),
            (((1,), (1,)), ((), ())),
            preferred_element_type=f32,
        )
        if u == 0:
            qkv[...] = piece
        else:
            qkv[...] += piece

    ends = jnp.zeros((1, 1), jnp.int32)
    ids_row = jnp.zeros((1, patches), jnp.int32)
    ids_col = jnp.zeros((patches, 1), jnp.int32)
    at_row = lax.broadcasted_iota(jnp.int32, (1, patches), 1)
    at_col = lax.broadcasted_iota(jnp.int32, (patches, 1), 0)
    for image in range(len_ref.shape[1]):
        ends = ends + len_ref[:, image : image + 1]
        ids_row = ids_row + (at_row >= ends * 4).astype(jnp.int32)
        ids_col = ids_col + (at_col >= ends * 4).astype(jnp.int32)
    same = ids_col == ids_row
    for head in range(heads_wide // HD):
        query, keys, values = (
            qkv[c * heads_wide + head * HD : c * heads_wide + (head + 1) * HD].astype(kind) for c in range(3)
        )
        scores = lax.dot_general(keys, query, (((0,), (0,)), ((), ())), preferred_element_type=f32) * HD ** (-0.5)
        scores = jnp.where(same, scores, -1e30)
        top = jnp.max(scores, axis=0, keepdims=True)
        expo = jnp.exp(scores - top)
        weights = (expo / jnp.sum(expo, axis=0, keepdims=True)).astype(kind)
        att[head * HD : (head + 1) * HD] = jnp.dot(values, weights, preferred_element_type=f32).astype(kind)
    loads["wp"].wait()
    total = ScatterSum(part, buf["r1"], buf["yb"], buf["r2"], sem)
    for u in range(2):
        piece = lax.dot_general(
            att[...], buf["wp"][:, u * half : (u + 1) * half], (((0,), (0,)), ((), ())), preferred_element_type=f32
        )
        part[u] = piece.astype(kind).reshape(m, own, half)
        total.start(u)
    for u in range(2):
        total.forward(u)
    for u in range(2):
        at = slice(u * half, (u + 1) * half)
        vo[:, at] = vit_ref[:, at].astype(f32) + total.finish(u)
    second = normalize(vo[...], gain2_ref[...])
    for k in range(width // 128):
        buf["vs"][k] = second[:, k * 128 : (k + 1) * 128]
    tokens = own // 4

    def merged_view(u, at):
        return ag2.at[u - 2, :, at]

    gather_two = LineGather(merged_view, sem)
    for q in range(2):
        for j in range(4):
            for k in range(half // 128):
                ag2[q, j, mt, :, k * 128 : (k + 1) * 128] = buf["vs"][
                    q * half // 128 + k, pl.ds(j, tokens, stride=4), :
                ].astype(kind)
        gather_two.start(q + 2)
    for k in range(1, m_a):
        for u in range(2):
            gather_two.relay(u + 2, k)
    loads["w1"].wait()
    expanded = None
    for u in range(2):
        gather_two.finish(u + 2)
        for j in range(4):
            at = j * width + u * half
            piece = jnp.dot(
                ag2[u, j].reshape(m * tokens, half), buf["w1"][at : at + half], preferred_element_type=f32
            )
            expanded = piece if expanded is None else expanded + piece
    out_ref[...] = (0.5 * expanded * (1.0 + lax.erf(expanded * 0.5**0.5))).astype(kind)


def vision(vit, lengths, gain, gain2, w_qkv, w_proj, w1, collective_id):
    m = lax.axis_size("tp")
    own, width = vit.shape
    half, kind, f32 = width // 2, vit.dtype, jnp.float32
    heads_wide = w_proj.shape[0]
    shapes = {
        "ag": ((2, m, own, half), kind),
        "wq": (w_qkv.shape, kind),
        "wp": (w_proj.shape, kind),
        "w1": (w1.shape, kind),
        "qkv": ((3 * heads_wide, m * own), f32),
        "att": ((heads_wide, m * own), kind),
        "vo": ((own, width), f32),
        "vs": ((width // 128, own, 128), f32),
        "ag2": ((2, 4, m, own // 4, half), kind),
    }
    shapes |= scatter_shapes(2, (own, half), kind)
    sems = {"wq": (), "wp": (), "w1": ()} | line_sems(4) | scatter_sems(2)
    anywhere = pl.BlockSpec(memory_space=pl.ANY)
    return pl.pallas_call(
        vision_kernel,
        out_shape=jax.ShapeDtypeStruct((m * own // 4, w1.shape[1]), kind),
        in_specs=[VM, VM, VM, VM, anywhere, anywhere, anywhere],
        out_specs=VM,
        scratch_shapes=[pltpu.VMEM(*shapes[k]) for k in V_BUFS]
        + [pltpu.SemaphoreType.DMA(sems[k]) if sems[k] else pltpu.SemaphoreType.DMA for k in V_SEMS],
        name="vision",
        compiler_params=pltpu.CompilerParams(
            collective_id=collective_id, has_side_effects=True, vmem_limit_bytes=60_000_000
        ),
    )(vit, lengths, gain, gain2, w_qkv, w_proj, w1)


SEMS = (
    "w2", "w", "d", "ea_s", "ea_r", "eb_s", "eb_r", "q_s", "q_r", "p_s", "p_r", "y_s", "y_r", "h_s", "h_r",
    "o_s", "b_r", "rb_s", "rb_r", "ra_s", "ra_r", "u_s", "u_r", "d_s", "d_r", "m_s", "m_r",
)
BUFS = (
    "ex", "w2s", "part", "r1", "yb", "r2", "tok", "nrm", "sqa", "rq", "inv", "held", "dheld", "gu", "pin",
    "keep", "yx", "rx", "hid", "acc",
)


def decoder_kernel(parts, e_ref, pos_ref, gain_ref, w2_ref, w_ref, d_ref, out_ref, *scratch):
    buf = dict(zip(BUFS, scratch))
    sem = dict(zip(SEMS, scratch[len(BUFS):]))
    n, m = lax.axis_size("seq"), lax.axis_size("tp")
    (n_a, n_b), (m_a, m_b) = factors(n), factors(m)
    me, mt = lax.axis_index("seq"), lax.axis_index("tp")
    a, b = me // n_b, lax.rem(me, n_b)
    ta, tb = mt // m_b, lax.rem(mt, m_b)
    x_peers, core_peers = grid_peers(n_a, n_b, a, b)
    t_major, t_minor = grid_peers(m_a, m_b, ta, tb)
    partner = core_peers[0]
    chunks, rows, depth = w_ref.shape[1:]
    steps = parts * chunks
    owned = steps // n_b
    count = n_a * 128
    block = count // m
    half = depth // 2

    def to(axis, src, dst, s, r, peer):
        return remote(src, dst, s, r, axis, peer)

    def lanes(owner):
        return pl.ds(pl.multiple_of(owner * 128, 128), 128)

    w2_load = pltpu.make_async_copy(
        w2_ref.at[:, pl.ds(pl.multiple_of(me * depth, depth), depth)], buf["w2s"], sem["w2"]
    )

    def w_load(i):
        slot = lax.rem(i, 2)
        return pltpu.make_async_copy(w_ref.at[:, lax.rem(i, chunks)], buf["held"].at[slot], sem["w"].at[slot])

    def d_load(i):
        slot = lax.rem(i, 2)
        return pltpu.make_async_copy(d_ref.at[lax.rem(i, chunks)], buf["dheld"].at[slot], sem["d"].at[slot])

    w2_load.start()
    w_load(0).start()

    barrier = pltpu.get_barrier_semaphore()
    everyone = [("seq", lax.rem(me + d, n)) for d in range(1, n)]
    everyone += [("tp", peer) for peer in t_major + t_minor]
    for axis, peer in everyone:
        pl.semaphore_signal(barrier, inc=1, device_id={axis: peer}, device_id_type=MESH)
    pl.semaphore_wait(barrier, len(everyone))

    ex = buf["ex"]
    e_a = [
        to("seq", e_ref, ex.at[me], sem["ea_s"].at[da - 1], sem["ea_r"].at[da - 1], x_peers[da - 1])
        for da in range(1, n_a)
    ]
    e_b = [to("seq", e_ref, ex.at[me], sem["eb_s"].at[0], sem["eb_r"].at[0], partner)]
    for copy in e_a + e_b:
        copy.start()
    ex[me] = e_ref[...]
    for da in range(1, n_a):
        e_a[da - 1].wait_recv()
        source = ex.at[lax.rem(a - da + n_a, n_a) * n_b + b]
        copy = to("seq", source, source, sem["eb_s"].at[da], sem["eb_r"].at[da], partner)
        copy.start()
        e_b.append(copy)
    for copy in e_b:
        copy.wait()
    for copy in e_a:
        copy.wait_send()

    part, tok = buf["part"], buf["tok"]
    sums = ScatterSum(part, buf["r1"], buf["yb"], buf["r2"], sem)
    tokens_of = LineGather(lambda u, at: tok.at[u, at], sem)

    def ag_start(u):
        tok[u, mt] = sums.finish(u).astype(tok.dtype)
        tokens_of.start(u)

    rq, inv, sqa, nrm = buf["rq"], buf["inv"], buf["sqa"], buf["nrm"]

    def squares(h, d):
        return to(
            "seq", rq.at[h, me], rq.at[h, me], sem["q_s"].at[h, d - 1], sem["q_r"].at[h, d - 1], lax.rem(me + d, n)
        )

    def ag_finish(h):
        tokens_of.finish(h)
        first = lax.rem(h, 2) * half

        def rows_of(t, carry):
            values = tok[h, t].astype(jnp.float32)
            at = pl.ds(pl.multiple_of(t * block, block), block)
            cols = pl.ds(pl.multiple_of(first, 128), half)
            nrm[at, cols] = (values * gain_ref[:, cols]).astype(nrm.dtype)
            total = values[:, :128] * values[:, :128]
            for k in range(1, half // 128):
                piece = values[:, k * 128 : (k + 1) * 128]
                total = total + piece * piece
            sqa[lax.rem(h, 2), at] = total
            return carry

        lax.fori_loop(0, m, rows_of, 0)

    def ag_both(h):
        ag_finish(2 * h)
        ag_finish(2 * h + 1)
        squared = jnp.sum(jnp.transpose(sqa[0] + sqa[1]), axis=0, keepdims=True)
        rq[h, me] = jnp.broadcast_to(squared, (8, count))
        for d in range(1, n):
            squares(h, d).start()

    def inverse(h):
        for d in range(1, n):
            squares(h, d).wait()
        total = rq[h, 0]
        for s in range(1, n):
            total = total + rq[h, s]
        inv[h] = lax.rsqrt(total / (depth * n) + 1e-06)

    w2_load.wait()
    for h in range(parts):
        row = lax.broadcasted_iota(jnp.int32, (count, pos_ref.shape[1]), 0)
        slot = lax.shift_right_logical(row, block.bit_length() - 1) * (block * (parts - 1)) + row + h * block
        pick = (slot == pos_ref[...]).astype(jnp.bfloat16)
        moved = jnp.dot(
            pick, ex[...].reshape(pos_ref.shape[1], ex.shape[2]), preferred_element_type=jnp.float32
        ).astype(jnp.bfloat16)
        width = min(512, half)
        for k in range(depth // width):
            piece = jnp.dot(
                moved, buf["w2s"][:, k * width : (k + 1) * width], preferred_element_type=jnp.float32
            ).astype(part.dtype)
            q, at = k * width // half, k * width % half
            part[2 * h + q, :, :, at : at + width] = piece.reshape(m, block, width)
            if h == 0 and at + width == half:
                sums.start(q)
    sums.forward(0)
    sums.forward(1)
    ag_start(0)
    ag_start(1)
    for k in range(1, m_a):
        for u in range(2):
            tokens_of.relay(u, k)
    if parts > 1:
        sums.start(2)
        sums.start(3)
    ag_both(0)

    gu, pin, keep, yx, rx, hid, acc = (buf[k] for k in ("gu", "pin", "keep", "yx", "rx", "hid", "acc"))

    def owner(i):
        return lax.rem(i, n_b) == b

    def to_owner(i):
        return to("seq", gu.at[lax.rem(i, 2)], pin.at[i // n_b], sem["p_s"].at[i // n_b], sem["p_r"].at[i // n_b], partner)

    def to_x(i, da):
        o = i // n_b
        return to(
            "seq", yx.at[o, da - 1], rx.at[o, da - 1], sem["y_s"].at[o, da - 1], sem["y_r"].at[o, da - 1], x_peers[da - 1]
        )

    def hid_x(i, da):
        target = hid.at[i, :, lanes(a)]
        return to("seq", target, target, sem["h_s"].at[i, da - 1], sem["h_r"].at[i, da - 1], x_peers[da - 1])

    def hid_core(i, da):
        target = hid.at[i, :, lanes(lax.rem(a - da + n_a, n_a))]
        return to("seq", target, target, sem["o_s"].at[i, da], sem["b_r"].at[i, da], partner)

    def stage_a(i):
        w_load(i).wait()

        @pl.when(i + 1 < steps)
        def _():
            w_load(i + 1).start()

        for half in range(2):
            gu[lax.rem(i, 2), half] = lax.dot_general(
                buf["held"][lax.rem(i, 2), half],
                nrm[...],
                (((1,), (1,)), ((), ())),
                preferred_element_type=jnp.float32,
            ).astype(gu.dtype)

        @pl.when(jnp.logical_not(owner(i)))
        def _():
            to_owner(i).start()

    def stage_b(i):
        o = i // n_b

        @pl.when(owner(i))
        def _():
            to_owner(i).wait_recv()

            def both(da):
                at = lanes(lax.rem(a + da, n_a))
                return gu[lax.rem(i, 2), :, :, at].astype(jnp.float32) + pin[o, :, :, at].astype(jnp.float32)

            for da in range(1, n_a):
                yx[o, da - 1] = both(da).astype(yx.dtype)
                to_x(i, da).start()
            keep[lax.rem(o, 2)] = both(0)

        @pl.when(jnp.logical_not(owner(i)))
        def _():
            to_owner(i).wait_send()

    def stage_c(i):
        o, h = i // n_b, i // chunks

        @pl.when(lax.rem(i, chunks) == 0)
        def _():
            inverse(h)

        @pl.when(owner(i))
        def _():
            total = keep[lax.rem(o, 2)]
            for da in range(1, n_a):
                to_x(i, da).wait()
                total = total + rx[o, da - 1].astype(jnp.float32)
            total = total * inv[h, 0:1, lanes(a)]
            hid[i, :, lanes(a)] = (jax.nn.silu(total[0]) * total[1]).astype(hid.dtype)
            for da in range(1, n_a):
                hid_x(i, da).start()
            hid_core(i, 0).start()

    def stage_d(i):
        @pl.when(owner(i))
        def _():
            for da in range(1, n_a):
                hid_x(i, da).wait()
                hid_core(i, da).start()

    def stage_e(i):
        c, h = lax.rem(i, chunks), i // chunks

        @pl.when(owner(i))
        def _():
            for da in range(n_a):
                hid_core(i, da).wait_send()

        @pl.when(jnp.logical_not(owner(i)))
        def _():
            for da in range(n_a):
                hid_core(i, da).wait_recv()

        d_load(i).wait()
        width = min(512, depth)
        left = hid[i]
        for k in range(depth // width):
            at = slice(k * width, (k + 1) * width)
            piece = lax.dot_general(
                left, buf["dheld"][lax.rem(i, 2), :, at], (((0,), (0,)), ((), ())), preferred_element_type=jnp.float32
            )

            @pl.when(c == 0)
            def _():
                acc[:, at] = piece

            @pl.when(c > 0)
            def _():
                acc[:, at] += piece

        @pl.when(c == chunks - 1)
        def _():
            for q in range(2):
                u = 2 * parts + 2 * h + q
                part[u] = acc[:, q * half : (q + 1) * half].astype(part.dtype).reshape(m, block, half)
                sums.start(u)

    def down_pass(h):
        sums.forward(2 * parts + 2 * h)
        sums.forward(2 * parts + 2 * h + 1)

    def output(h):
        at = pl.ds(pl.multiple_of(h * block, block), block)
        for q in range(2):
            total = sums.finish(2 * parts + 2 * h + q)
            out_ref[at, q * half : (q + 1) * half] = (
                tok[2 * h + q, mt].astype(jnp.float32) + total
            ).astype(out_ref.dtype)

    def iteration(i, carry):
        def when(lag, fn):
            @pl.when(jnp.logical_and(i >= lag, i - lag < steps))
            def _():
                fn(i - lag)

        h, k = i // chunks, lax.rem(i, chunks)
        more = h + 1 < parts

        def at_step(step, q, fn):
            @pl.when(jnp.logical_and(more, k == step * chunks // 7))
            def _():
                fn(2 * h + 2 + q)

        @pl.when(jnp.logical_and(jnp.logical_and(i > 0, i < steps), k == 0))
        def _():
            @pl.when(more)
            def _():
                sums.start(2 * h + 2)
                sums.start(2 * h + 3)

            ag_both(h)

        when(LAG_E - 1, lambda j: d_load(j).start())
        when(0, stage_a)
        when(1, stage_b)
        when(LAG_C, stage_c)
        when(LAG_D, stage_d)
        for q in range(2):
            at_step(AT_PASS[q], q, sums.forward)
        for q in range(2):
            at_step(AT_GATHER[q], q, ag_start)
        for hop in range(1, m_a):
            for q in range(2):
                at_step(AT_RELAY[min(hop - 1, 2)], q, lambda u, hop=hop: tokens_of.relay(u, hop))
        when(LAG_E, stage_e)

        def later(lag, fn):
            @pl.when(jnp.logical_and(i - lag >= chunks, jnp.logical_and(lax.rem(i - lag + chunks, chunks) == 0, i - lag < steps)))
            def _():
                fn((i - lag) // chunks - 1)

        later(LAG_E + 1, down_pass)
        later(LAG_E + 3, output)
        return carry

    lax.fori_loop(0, steps + LAG_E, iteration, 0)
    down_pass(parts - 1)
    output(parts - 1)


def decoder(expanded, positions, gain, w2, weight, down, collective_id):
    n, m = lax.axis_size("seq"), lax.axis_size("tp")
    (n_a, n_b), (m_a, m_b) = factors(n), factors(m)
    _, chunks, rows, depth = weight.shape
    tokens = positions.shape[1]
    count = n_a * 128
    parts = tokens // count
    steps = parts * chunks
    block = count // m
    assert n_b == 2 and steps % 2 == 0 and chunks >= 7
    kind, f32 = expanded.dtype, jnp.float32
    shapes = {
        "ex": ((n,) + expanded.shape, kind),
        "w2s": ((w2.shape[0], depth), kind),
        "tok": ((2 * parts, m, block, depth // 2), kind),
        "nrm": ((count, depth), kind),
        "sqa": ((2, count, 128), f32),
        "rq": ((parts, n, 8, count), f32),
        "inv": ((parts, 8, count), f32),
        "held": ((2, 2, rows, depth), kind),
        "dheld": ((2, rows, depth), kind),
        "gu": ((2, 2, rows, count), kind),
        "pin": ((steps // 2, 2, rows, count), kind),
        "keep": ((2, 2, rows, 128), f32),
        "yx": ((steps // 2, n_a - 1, 2, rows, 128), kind),
        "rx": ((steps // 2, n_a - 1, 2, rows, 128), kind),
        "hid": ((steps, rows, count), kind),
        "acc": ((count, depth), f32),
    }
    shapes |= scatter_shapes(4 * parts, (block, depth // 2), kind)
    sems = {
        "w2": (),
        "w": (2,),
        "d": (2,),
        "ea_s": (n_a,),
        "ea_r": (n_a,),
        "eb_s": (n_a,),
        "eb_r": (n_a,),
        "q_s": (parts, n),
        "q_r": (parts, n),
        "p_s": (steps // 2,),
        "p_r": (steps // 2,),
        "y_s": (steps // 2, n_a),
        "y_r": (steps // 2, n_a),
        "h_s": (steps, n_a),
        "h_r": (steps, n_a),
        "o_s": (steps, n_a),
        "b_r": (steps, n_a),
    }
    sems |= scatter_sems(4 * parts) | line_sems(2 * parts)
    anywhere = pl.BlockSpec(memory_space=pl.ANY)
    return pl.pallas_call(
        functools.partial(decoder_kernel, parts),
        out_shape=jax.ShapeDtypeStruct((tokens // m, depth), kind),
        in_specs=[VM, VM, VM, anywhere, anywhere, anywhere],
        out_specs=VM,
        scratch_shapes=[pltpu.VMEM(*shapes[k]) for k in BUFS]
        + [pltpu.SemaphoreType.DMA(sems[k]) if sems[k] else pltpu.SemaphoreType.DMA for k in SEMS],
        name="decoder",
        compiler_params=pltpu.CompilerParams(
            collective_id=collective_id, has_side_effects=True, vmem_limit_bytes=67_000_000
        ),
    )(expanded, positions, gain, w2, weight, down)


def chunk_count(rows):
    for count in (7, 6, 4, 3, 2):
        if rows % (count * 8) == 0:
            return count
    return 1


def local(
    vit_input,
    image_lengths,
    positions,
    vit_ln_gain,
    w_qkv,
    w_proj,
    merger_ln_gain,
    merger_w1,
    merger_w2,
    norm_gain,
    gate_up_weight,
    down_weight,
):
    width, _, head_cols = w_qkv.shape
    expanded = vision(
        vit_input,
        image_lengths,
        vit_ln_gain[None, :],
        merger_ln_gain[None, :],
        w_qkv.transpose(1, 2, 0).reshape(3 * head_cols, width),
        w_proj,
        merger_w1,
        0,
    )
    slice_width = norm_gain.shape[0]
    hidden_width = gate_up_weight.shape[2]
    chunks = chunk_count(hidden_width)
    weight_rows = gate_up_weight.transpose(1, 2, 0).reshape(
        2, chunks, hidden_width // chunks, slice_width
    )
    down_rows = down_weight.reshape(chunks, hidden_width // chunks, slice_width)
    return decoder(
        expanded, positions[None, :], norm_gain[None, :], merger_w2, weight_rows, down_rows, 3
    )


def solution(mesh):
    return jax.shard_map(
        local,
        mesh=mesh,
        in_specs=(
            P(("seq", "tp"), None),
            P("seq", None),
            P(),
            P(),
            P(None, None, "tp"),
            P("tp", None),
            P(),
            P(None, "tp"),
            P("tp", None),
            P("seq"),
            P("seq", None, "tp"),
            P("tp", "seq"),
        ),
        out_specs=P("tp", "seq"),
        check_vma=False,
    )
```

```python
import functools

import jax
import jax.numpy as jnp
from jax import lax
from jax.experimental import pallas as pl
from jax.experimental.pallas import tpu as pltpu
from jax.sharding import PartitionSpec as P

HD = 80
MESH = pl.DeviceIdType.MESH
LAG_C, LAG_D, LAG_E = 3, 5, 6
AT_PASS, AT_GATHER, AT_RELAY = (0, 1), (2, 3), (2, 3)
VM = pl.BlockSpec(memory_space=pltpu.VMEM)


def factors(n):
    minor = max(d for d in range(1, n + 1) if n % d == 0 and d * d <= n)
    return n // minor, minor


def grid_peers(n_a, n_b, a, b):
    along_a = [lax.rem(a + da, n_a) * n_b + b for da in range(1, n_a)]
    along_b = [a * n_b + lax.rem(b + db, n_b) for db in range(1, n_b)]
    return along_a, along_b


def remote(src, dst, send_sem, recv_sem, axis, peer):
    return pltpu.make_async_remote_copy(
        src_ref=src,
        dst_ref=dst,
        send_sem=send_sem,
        recv_sem=recv_sem,
        device_id={axis: peer},
        device_id_type=MESH,
    )


class LineGather:
    def __init__(self, view, sems):
        n = lax.axis_size("tp")
        self.n_a, self.n_b = factors(n)
        me = lax.axis_index("tp")
        self.a, self.b = me // self.n_b, lax.rem(me, self.n_b)
        self.minors = grid_peers(self.n_a, self.n_b, self.a, self.b)[1]
        self.view, self.sems = view, sems

    def up(self, u, src):
        block = self.view(u, src * self.n_b + self.b)
        send, recv = self.sems["u_s"].at[u, src], self.sems["u_r"].at[u, src]
        return remote(block, block, send, recv, "tp", lax.rem(self.a + 1, self.n_a) * self.n_b + self.b)

    def down(self, u, src):
        block = self.view(u, src * self.n_b + self.b)
        send, recv = self.sems["d_s"].at[u, src], self.sems["d_r"].at[u, src]
        return remote(block, block, send, recv, "tp", lax.rem(self.a + self.n_a - 1, self.n_a) * self.n_b + self.b)

    def minor(self, u, src, db):
        block = self.view(u, src * self.n_b + self.b)
        send, recv = self.sems["m_s"].at[u, src, db - 1], self.sems["m_r"].at[u, src, db - 1]
        return remote(block, block, send, recv, "tp", self.minors[db - 1])

    def send(self, u, src, upward, downward):
        if upward:
            @pl.when(self.a < self.n_a - 1)
            def _():
                self.up(u, src).start()
        if downward:
            @pl.when(self.a > 0)
            def _():
                self.down(u, src).start()
        for db in range(1, self.n_b):
            self.minor(u, src, db).start()

    def start(self, u):
        self.send(u, self.a, True, True)

    def relay(self, u, k):
        @pl.when(self.a >= k)
        def _():
            self.up(u, self.a - k).wait_recv()
            self.send(u, self.a - k, True, False)

        @pl.when(self.a + k < self.n_a)
        def _():
            self.down(u, self.a + k).wait_recv()
            self.send(u, self.a + k, False, True)

    def finish(self, u):
        for src in range(self.n_a):
            for db in range(1, self.n_b):
                self.minor(u, src, db).wait()

            @pl.when(jnp.logical_and(src <= self.a, self.a < self.n_a - 1))
            def _():
                self.up(u, src).wait_send()

            @pl.when(jnp.logical_and(src >= self.a, self.a > 0))
            def _():
                self.down(u, src).wait_send()


def line_sems(units):
    m_a, m_b = factors(lax.axis_size("tp"))
    return {
        "u_s": (units, m_a), "u_r": (units, m_a), "d_s": (units, m_a), "d_r": (units, m_a),
        "m_s": (units, m_a, m_b), "m_r": (units, m_a, m_b),
    }


class ScatterSum:
    def __init__(self, part, r1, yb, r2, sems):
        m = lax.axis_size("tp")
        self.n_a, self.n_b = factors(m)
        me = lax.axis_index("tp")
        self.a, self.b = me // self.n_b, lax.rem(me, self.n_b)
        self.majors, self.minors = grid_peers(self.n_a, self.n_b, self.a, self.b)
        self.part, self.r1, self.yb, self.r2, self.sems = part, r1, yb, r2, sems
        self.order = sorted(range(1, self.n_a), key=lambda da: -min(da, self.n_a - da)) + [0]

    def slot(self, u):
        return lax.rem(u, self.part.shape[0])

    def minor(self, u, da, db):
        at = lax.rem(self.a + da, self.n_a) * self.n_b + lax.rem(self.b + db, self.n_b)
        send, recv = self.sems["rb_s"].at[u, da, db - 1], self.sems["rb_r"].at[u, da, db - 1]
        return remote(self.part.at[self.slot(u), at], self.r1.at[u, da, db - 1], send, recv, "tp", self.minors[db - 1])

    def major(self, u, da):
        send, recv = self.sems["ra_s"].at[u, da - 1], self.sems["ra_r"].at[u, da - 1]
        return remote(self.yb.at[self.slot(u), da - 1], self.r2.at[u, da - 1], send, recv, "tp", self.majors[da - 1])

    def start(self, u):
        for da in self.order:
            for db in range(1, self.n_b):
                self.minor(u, da, db).start()

    def arrived(self, u, da):
        total = self.part[self.slot(u), lax.rem(self.a + da, self.n_a) * self.n_b + self.b].astype(jnp.float32)
        for db in range(1, self.n_b):
            self.minor(u, da, db).wait_recv()
            total = total + self.r1[u, da, db - 1].astype(jnp.float32)
        return total

    def forward(self, u):
        for da in self.order[:-1]:
            self.yb[self.slot(u), da - 1] = self.arrived(u, da).astype(self.yb.dtype)
            self.major(u, da).start()

    def finish(self, u):
        total = self.arrived(u, 0)
        for da in self.order[:-1]:
            self.major(u, da).wait_recv()
            total = total + self.r2[u, da - 1].astype(jnp.float32)
        for da in self.order:
            for db in range(1, self.n_b):
                self.minor(u, da, db).wait_send()
        for da in self.order[:-1]:
            self.major(u, da).wait_send()
        return total


def scatter_sems(units):
    m_a, m_b = factors(lax.axis_size("tp"))
    return {"rb_s": (units, m_a, m_b), "rb_r": (units, m_a, m_b), "ra_s": (units, m_a), "ra_r": (units, m_a)}


def scatter_shapes(units, slots, block, kind):
    m_a, m_b = factors(lax.axis_size("tp"))
    return {
        "part": ((slots, m_a * m_b) + block, kind),
        "r1": ((units, m_a, m_b - 1) + block, kind),
        "yb": ((slots, m_a - 1) + block, kind),
        "r2": ((units, m_a - 1) + block, kind),
    }


def lane_rows(vector):
    return vector.reshape(-1, 128)


def one_row(ref, first=0, count=None):
    count = ref.shape[0] if count is None else count
    return jnp.concatenate([ref[pl.ds(first + k, 1)] for k in range(count)], axis=1)


def normalize(values, gain):
    mean = jnp.mean(values, axis=-1, keepdims=True)
    centered = values - mean
    variance = jnp.mean(centered * centered, axis=-1, keepdims=True)
    return centered * lax.rsqrt(variance + 1e-06) * gain


def keyed(prefix, named):
    return {prefix + k: v for k, v in named.items()}


def under(prefix, named):
    return {k[len(prefix):]: v for k, v in named.items() if k.startswith(prefix)}


def vision_stage(vit_ref, len_ref, gain_ref, gain2_ref, loads, buf, sem, enter, emit):
    m = lax.axis_size("tp")
    m_a, m_b = factors(m)
    mt = lax.axis_index("tp")
    own, width = vit_ref.shape
    half = width // 2
    heads_wide = buf["wp"].shape[0]
    f32, kind = jnp.float32, vit_ref.dtype
    ag, ag2, vo, part, qkv, att = (buf[k] for k in ("ag", "ag2", "vo", "part", "qkv", "att"))
    first = normalize(vit_ref[...].astype(f32), one_row(gain_ref)).astype(kind)
    for q in range(2):
        ag[q, mt] = first[:, q * half : (q + 1) * half]
    enter()

    def unit_view(u, at):
        return ag.at[u, at]

    gather_one = LineGather(unit_view, sem)
    for u in range(2):
        gather_one.start(u)
    for k in range(1, m_a):
        for u in range(2):
            gather_one.relay(u, k)
    loads["wq"].wait()
    patches = m * own
    for u in range(2):
        gather_one.finish(u)
        piece = lax.dot_general(
            buf["wq"][:, u * half : (u + 1) * half],
            ag[u].reshape(patches, half),
            (((1,), (1,)), ((), ())),
            preferred_element_type=f32,
        )
        if u == 0:
            qkv[...] = piece
        else:
            qkv[...] += piece

    ends = jnp.zeros((1, 1), jnp.int32)
    ids_row = jnp.zeros((1, patches), jnp.int32)
    ids_col = jnp.zeros((patches, 1), jnp.int32)
    at_row = lax.broadcasted_iota(jnp.int32, (1, patches), 1)
    at_col = lax.broadcasted_iota(jnp.int32, (patches, 1), 0)
    for image in range(len_ref.shape[1]):
        ends = ends + len_ref[:, image : image + 1]
        ids_row = ids_row + (at_row >= ends * 4).astype(jnp.int32)
        ids_col = ids_col + (at_col >= ends * 4).astype(jnp.int32)
    same = ids_col == ids_row
    for head in range(heads_wide // HD):
        query, keys, values = (
            qkv[c * heads_wide + head * HD : c * heads_wide + (head + 1) * HD].astype(kind) for c in range(3)
        )
        scores = lax.dot_general(keys, query, (((0,), (0,)), ((), ())), preferred_element_type=f32) * HD ** (-0.5)
        scores = jnp.where(same, scores, -1e30)
        top = jnp.max(scores, axis=0, keepdims=True)
        expo = jnp.exp(scores - top)
        weights = (expo / jnp.sum(expo, axis=0, keepdims=True)).astype(kind)
        att[head * HD : (head + 1) * HD] = jnp.dot(values, weights, preferred_element_type=f32).astype(kind)
    loads["wp"].wait()
    total = ScatterSum(part, buf["r1"], buf["yb"], buf["r2"], sem)
    for u in range(2):
        piece = lax.dot_general(
            att[...], buf["wp"][:, u * half : (u + 1) * half], (((0,), (0,)), ((), ())), preferred_element_type=f32
        )
        part[u] = piece.astype(kind).reshape(m, own, half)
        total.start(u)
    for u in range(2):
        total.forward(u)
    for u in range(2):
        at = slice(u * half, (u + 1) * half)
        vo[:, at] = vit_ref[:, at].astype(f32) + total.finish(u)
    second = normalize(vo[...], one_row(gain2_ref))
    for k in range(width // 128):
        buf["vs"][k] = second[:, k * 128 : (k + 1) * 128]
    tokens = own // 4

    def merged_view(u, at):
        return ag2.at[u - 2, :, at]

    gather_two = LineGather(merged_view, sem)
    for q in range(2):
        for j in range(4):
            for k in range(half // 128):
                ag2[q, j, mt, :, k * 128 : (k + 1) * 128] = buf["vs"][
                    q * half // 128 + k, pl.ds(j, tokens, stride=4), :
                ].astype(kind)
        gather_two.start(q + 2)
    for k in range(1, m_a):
        for u in range(2):
            gather_two.relay(u + 2, k)
    loads["w1"].wait()
    for u in range(2):
        gather_two.finish(u + 2)
    for piece, (start, stop) in enumerate(pieces_of(buf["w1"].shape[1])):
        expanded = None
        for u in range(2):
            for j in range(4):
                at = j * width + u * half
                term = jnp.dot(
                    ag2[u, j].reshape(m * tokens, half),
                    buf["w1"][at : at + half, start:stop],
                    preferred_element_type=f32,
                )
                expanded = term if expanded is None else expanded + term
        emit(piece, (0.5 * expanded * (1.0 + lax.erf(expanded * 0.5**0.5))).astype(kind))


def pieces_of(width):
    middle = -(-width // 256) * 128
    return [(0, middle), (middle, width)]


def vision_parts(own, width, heads_wide, hidden, kind):
    m, half, f32 = lax.axis_size("tp"), width // 2, jnp.float32
    shapes = {
        "ag": ((2, m, own, half), kind),
        "wq": ((3 * heads_wide, width), kind),
        "wp": ((heads_wide, width), kind),
        "w1": ((4 * width, hidden), kind),
        "qkv": ((3 * heads_wide, m * own), f32),
        "att": ((heads_wide, m * own), kind),
        "vo": ((own, width), f32),
        "vs": ((width // 128, own, 128), f32),
        "ag2": ((2, 4, m, own // 4, half), kind),
    }
    shapes |= scatter_shapes(2, 2, (own, half), kind)
    return shapes, {"wq": (), "wp": (), "w1": ()} | line_sems(4) | scatter_sems(2)


def step_kernel(
    parts, buf_names, sem_names, first_local, later_local, vit_ref, len_ref, vgain_ref, mgain_ref, pos_ref, gain_ref,
    wq_ref, wp_ref, w1_ref, w2_ref, w_ref, d_ref, out_ref, *scratch
):
    buf = dict(zip(buf_names, scratch))
    sem = dict(zip(sem_names, scratch[len(buf_names):]))
    n, m = lax.axis_size("seq"), lax.axis_size("tp")
    (n_a, n_b), (m_a, m_b) = factors(n), factors(m)
    me, mt = lax.axis_index("seq"), lax.axis_index("tp")
    a, b = me // n_b, lax.rem(me, n_b)
    ta, tb = mt // m_b, lax.rem(mt, m_b)
    x_peers, core_peers = grid_peers(n_a, n_b, a, b)
    t_major, t_minor = grid_peers(m_a, m_b, ta, tb)
    partner = core_peers[0]
    chunks, rows, depth = w_ref.shape[1:]
    steps = parts * chunks
    owned = steps // n_b
    count = n_a * 128
    block = count // m
    half = depth // 2
    tokens = parts * count
    places = one_row(pos_ref)

    def to(axis, src, dst, s, r, peer):
        return remote(src, dst, s, r, axis, peer)

    def lanes(owner):
        return pl.ds(pl.multiple_of(owner * 128, 128), 128)

    w2_load = pltpu.make_async_copy(
        w2_ref.at[:, pl.ds(pl.multiple_of(me * depth, depth), depth)], buf["w2s"], sem["w2"]
    )

    def w_load(i):
        slot = lax.rem(i, 2)
        return pltpu.make_async_copy(w_ref.at[:, lax.rem(i, chunks)], buf["held"].at[slot], sem["w"].at[slot])

    def d_load(i):
        slot = lax.rem(i, 2)
        return pltpu.make_async_copy(d_ref.at[lax.rem(i, chunks)], buf["dheld"].at[slot], sem["d"].at[slot])


    barrier = pltpu.get_barrier_semaphore()
    everyone = [("seq", lax.rem(me + d, n)) for d in range(1, n)]
    everyone += [("tp", peer) for peer in t_major + t_minor]

    def enter():
        pl.semaphore_wait(barrier, len(everyone))

    ex = buf["ex"]
    columns = [pl.ds(start, stop - start) for start, stop in pieces_of(ex.shape[2])]

    def ex_x(piece, da):
        own = ex.at[me, :, columns[piece]]
        return to("seq", own, own, sem["ea_s"].at[piece, da - 1], sem["ea_r"].at[piece, da - 1], x_peers[da - 1])

    def ex_core(piece, da):
        held = ex.at[lax.rem(a - da + n_a, n_a) * n_b + b, :, columns[piece]]
        return to("seq", held, held, sem["eb_s"].at[piece, da], sem["eb_r"].at[piece, da], partner)

    def emit(piece, values):
        ex[me, :, columns[piece]] = values
        for da in range(1, n_a):
            ex_x(piece, da).start()
        ex_core(piece, 0).start()

    def first_half(**own):
        loads = {
            k: pltpu.make_async_copy(ref, own["v_" + k], sem["v_" + k])
            for k, ref in (("wq", wq_ref), ("wp", wp_ref), ("w1", w1_ref))
        }
        for copy in loads.values():
            copy.start()
        w2_load.start()
        w_load(0).start()
        for axis, peer in everyone:
            pl.semaphore_signal(barrier, inc=1, device_id={axis: peer}, device_id_type=MESH)
        vision_stage(
            vit_ref, len_ref, vgain_ref, mgain_ref, loads, under("v_", buf | own), under("v_", sem), enter, emit
        )

    pl.run_scoped(first_half, **{k: pltpu.VMEM(*v) for k, v in first_local.items()})
    for piece in range(2):
        for da in range(1, n_a):
            ex_x(piece, da).wait_recv()
            ex_core(piece, da).start()
    for piece in range(2):
        for da in range(n_a):
            ex_core(piece, da).wait()
        for da in range(1, n_a):
            ex_x(piece, da).wait_send()

    def second_half(**own):
        buf.update(own)
        part, tok = buf["part"], buf["tok"]
        sums = ScatterSum(part, buf["r1"], buf["yb"], buf["r2"], sem)
        tokens_of = LineGather(lambda u, at: tok.at[u, at], sem)

        def ag_start(u):
            tok[u, mt] = sums.finish(u).astype(tok.dtype)
            tokens_of.start(u)

        rq, inv, sqa, nrm = buf["rq"], buf["inv"], buf["sqa"], buf["nrm"]

        def squares(h, d):
            return to(
                "seq", rq.at[h, me], rq.at[h, me], sem["q_s"].at[h, d - 1], sem["q_r"].at[h, d - 1], lax.rem(me + d, n)
            )

        def ag_finish(h):
            tokens_of.finish(h)
            first = lax.rem(h, 2) * half
            gain = one_row(gain_ref, lax.rem(h, 2) * (half // 128), half // 128)

            def rows_of(t, carry):
                values = tok[h, t].astype(jnp.float32)
                at = pl.ds(pl.multiple_of(t * block, block), block)
                cols = pl.ds(pl.multiple_of(first, 128), half)
                nrm[at, cols] = (values * gain).astype(nrm.dtype)
                total = values[:, :128] * values[:, :128]
                for k in range(1, half // 128):
                    piece = values[:, k * 128 : (k + 1) * 128]
                    total = total + piece * piece
                sqa[lax.rem(h, 2), at] = total
                return carry

            lax.fori_loop(0, m, rows_of, 0)

        def ag_both(h):
            ag_finish(2 * h)
            ag_finish(2 * h + 1)
            squared = jnp.sum(jnp.transpose(sqa[0] + sqa[1]), axis=0, keepdims=True)
            rq[h, me] = jnp.broadcast_to(squared, (8, count))
            for d in range(1, n):
                squares(h, d).start()

        def inverse(h):
            for d in range(1, n):
                squares(h, d).wait()
            total = rq[h, 0]
            for s in range(1, n):
                total = total + rq[h, s]
            inv[h] = lax.rsqrt(total / (depth * n) + 1e-06)

        w2_load.wait()
        for h in range(parts):
            row = lax.broadcasted_iota(jnp.int32, (count, tokens), 0)
            slot = lax.shift_right_logical(row, block.bit_length() - 1) * (block * (parts - 1)) + row + h * block
            pick = (slot == places).astype(jnp.bfloat16)
            moved = jnp.dot(
                pick, ex[...].reshape(tokens, ex.shape[2]), preferred_element_type=jnp.float32
            ).astype(jnp.bfloat16)
            width = min(512, half)
            for k in range(depth // width):
                piece = jnp.dot(
                    moved, buf["w2s"][:, k * width : (k + 1) * width], preferred_element_type=jnp.float32
                ).astype(part.dtype)
                q, at = k * width // half, k * width % half
                part[2 * h + q, :, :, at : at + width] = piece.reshape(m, block, width)
                if h == 0 and at + width == half:
                    sums.start(q)
        sums.forward(0)
        sums.forward(1)
        if parts > 1:
            sums.start(2)
        ag_start(0)
        ag_start(1)
        for k in range(1, m_a):
            for u in range(2):
                tokens_of.relay(u, k)
        if parts > 1:
            sums.start(3)
        ag_both(0)

        gu, pin, keep, yx, rx, hid, acc = (buf[k] for k in ("gu", "pin", "keep", "yx", "rx", "hid", "acc"))

        def owner(i):
            return lax.rem(i, n_b) == b

        def to_owner(i):
            return to("seq", gu.at[lax.rem(i, 2)], pin.at[i // n_b], sem["p_s"].at[i // n_b], sem["p_r"].at[i // n_b], partner)

        def to_x(i, da):
            o = i // n_b
            return to(
                "seq", yx.at[lax.rem(o, 4), da - 1], rx.at[o, da - 1], sem["y_s"].at[o, da - 1], sem["y_r"].at[o, da - 1], x_peers[da - 1]
            )

        def hid_x(i, da):
            target = hid.at[i, :, lanes(a)]
            return to("seq", target, target, sem["h_s"].at[i, da - 1], sem["h_r"].at[i, da - 1], x_peers[da - 1])

        def hid_core(i, da):
            target = hid.at[i, :, lanes(lax.rem(a - da + n_a, n_a))]
            return to("seq", target, target, sem["o_s"].at[i, da], sem["b_r"].at[i, da], partner)

        def stage_a(i):
            w_load(i).wait()

            @pl.when(i + 1 < steps)
            def _():
                w_load(i + 1).start()

            for half in range(2):
                gu[lax.rem(i, 2), half] = lax.dot_general(
                    buf["held"][lax.rem(i, 2), half],
                    nrm[...],
                    (((1,), (1,)), ((), ())),
                    preferred_element_type=jnp.float32,
                ).astype(gu.dtype)

            @pl.when(jnp.logical_not(owner(i)))
            def _():
                to_owner(i).start()

        def stage_b(i):
            o = i // n_b

            @pl.when(owner(i))
            def _():
                to_owner(i).wait_recv()

                def both(da):
                    at = lanes(lax.rem(a + da, n_a))
                    return gu[lax.rem(i, 2), :, :, at].astype(jnp.float32) + pin[o, :, :, at].astype(jnp.float32)

                for da in range(1, n_a):
                    yx[lax.rem(o, 4), da - 1] = both(da).astype(yx.dtype)
                    to_x(i, da).start()
                keep[lax.rem(o, 2)] = both(0)

            @pl.when(jnp.logical_not(owner(i)))
            def _():
                to_owner(i).wait_send()

        def stage_c(i):
            o, h = i // n_b, i // chunks

            @pl.when(lax.rem(i, chunks) == 0)
            def _():
                inverse(h)

            @pl.when(owner(i))
            def _():
                total = keep[lax.rem(o, 2)]
                for da in range(1, n_a):
                    to_x(i, da).wait()
                    total = total + rx[o, da - 1].astype(jnp.float32)
                total = total * inv[h, 0:1, lanes(a)]
                hid[i, :, lanes(a)] = (jax.nn.silu(total[0]) * total[1]).astype(hid.dtype)
                for da in range(1, n_a):
                    hid_x(i, da).start()
                hid_core(i, 0).start()

        def stage_d(i):
            @pl.when(owner(i))
            def _():
                for da in range(1, n_a):
                    hid_x(i, da).wait()
                    hid_core(i, da).start()

        def stage_e(i):
            c, h = lax.rem(i, chunks), i // chunks

            @pl.when(owner(i))
            def _():
                for da in range(n_a):
                    hid_core(i, da).wait_send()

            @pl.when(jnp.logical_not(owner(i)))
            def _():
                for da in range(n_a):
                    hid_core(i, da).wait_recv()

            d_load(i).wait()
            width = min(512, depth)
            left = hid[i]
            for k in range(depth // width):
                at = slice(k * width, (k + 1) * width)
                piece = lax.dot_general(
                    left, buf["dheld"][lax.rem(i, 2), :, at], (((0,), (0,)), ((), ())), preferred_element_type=jnp.float32
                )

                @pl.when(c == 0)
                def _():
                    acc[:, at] = piece

                @pl.when(c > 0)
                def _():
                    acc[:, at] += piece

            @pl.when(c == chunks - 1)
            def _():
                for q in range(2):
                    u = 2 * parts + 2 * h + q
                    part[2 * h + q] = acc[:, q * half : (q + 1) * half].astype(part.dtype).reshape(m, block, half)
                    sums.start(u)

        def down_pass(h):
            sums.forward(2 * parts + 2 * h)
            sums.forward(2 * parts + 2 * h + 1)

        def output(h):
            at = pl.ds(pl.multiple_of(h * block, block), block)
            for q in range(2):
                total = sums.finish(2 * parts + 2 * h + q)
                out_ref[at, q * half : (q + 1) * half] = (
                    tok[2 * h + q, mt].astype(jnp.float32) + total
                ).astype(out_ref.dtype)

        def iteration(i, carry):
            def when(lag, fn):
                @pl.when(jnp.logical_and(i >= lag, i - lag < steps))
                def _():
                    fn(i - lag)

            h, k = i // chunks, lax.rem(i, chunks)
            more = h + 1 < parts

            def at_step(step, q, fn):
                @pl.when(jnp.logical_and(more, k == step * chunks // 7))
                def _():
                    fn(2 * h + 2 + q)

            @pl.when(jnp.logical_and(jnp.logical_and(i > 0, i < steps), k == 0))
            def _():
                @pl.when(more)
                def _():
                    sums.start(2 * h + 2)
                    sums.start(2 * h + 3)

                ag_both(h)

            when(LAG_E - 1, lambda j: d_load(j).start())
            when(0, stage_a)
            when(1, stage_b)
            when(LAG_C, stage_c)
            when(LAG_D, stage_d)
            for q in range(2):
                at_step(AT_PASS[q], q, sums.forward)
            for q in range(2):
                at_step(AT_GATHER[q], q, ag_start)
            for hop in range(1, m_a):
                for q in range(2):
                    at_step(AT_RELAY[q] + hop, q, lambda u, hop=hop: tokens_of.relay(u, hop))
            when(LAG_E, stage_e)

            def later(lag, fn):
                @pl.when(jnp.logical_and(i - lag >= chunks, jnp.logical_and(lax.rem(i - lag + chunks, chunks) == 0, i - lag < steps)))
                def _():
                    fn((i - lag) // chunks - 1)

            later(LAG_E + 1, down_pass)
            later(LAG_E + 3, output)
            return carry

        lax.fori_loop(0, steps + LAG_E, iteration, 0)
        down_pass(parts - 1)
        output(parts - 1)

    pl.run_scoped(second_half, **{k: pltpu.VMEM(*v) for k, v in later_local.items()})


def whole_step(vit, lengths, vgain, mgain, positions, gain, w_qkv, w_proj, w1, w2, weight, down):
    n, m = lax.axis_size("seq"), lax.axis_size("tp")
    (n_a, n_b), (m_a, m_b) = factors(n), factors(m)
    _, chunks, rows, depth = weight.shape
    tokens = positions.size
    count = n_a * 128
    parts = tokens // count
    steps = parts * chunks
    block = count // m
    assert n_b == 2 and steps % 2 == 0 and chunks >= 7
    kind, f32 = vit.dtype, jnp.float32
    own, width = vit.shape
    group = m * own // 4
    shapes = {
        "ex": ((n, group, w1.shape[1]), kind),
        "w2s": ((w2.shape[0], depth), kind),
        "tok": ((2 * parts, m, block, depth // 2), kind),
        "nrm": ((count, depth), kind),
        "sqa": ((2, count, 128), f32),
        "rq": ((parts, n, 8, count), f32),
        "inv": ((parts, 8, count), f32),
        "held": ((2, 2, rows, depth), kind),
        "dheld": ((2, rows, depth), kind),
        "gu": ((2, 2, rows, count), kind),
        "pin": ((steps // 2, 2, rows, count), kind),
        "keep": ((2, 2, rows, 128), f32),
        "yx": ((4, n_a - 1, 2, rows, 128), kind),
        "rx": ((steps // 2, n_a - 1, 2, rows, 128), kind),
        "hid": ((steps, rows, count), kind),
        "acc": ((count, depth), f32),
    }
    shapes |= scatter_shapes(4 * parts, 2 * parts, (block, depth // 2), kind)
    sems = {
        "w2": (),
        "w": (2,),
        "d": (2,),
        "ea_s": (2, n_a),
        "ea_r": (2, n_a),
        "eb_s": (2, n_a),
        "eb_r": (2, n_a),
        "q_s": (parts, n),
        "q_r": (parts, n),
        "p_s": (steps // 2,),
        "p_r": (steps // 2,),
        "y_s": (steps // 2, n_a),
        "y_r": (steps // 2, n_a),
        "h_s": (steps, n_a),
        "h_r": (steps, n_a),
        "o_s": (steps, n_a),
        "b_r": (steps, n_a),
    }
    sems |= scatter_sems(4 * parts) | line_sems(2 * parts)
    v_shapes, v_sems = vision_parts(own, width, w_proj.shape[0], w1.shape[1], kind)
    shapes |= keyed("v_", v_shapes)
    sems |= keyed("v_", v_sems)
    first = ("v_wq", "v_wp", "v_w1", "v_qkv", "v_att", "v_vo", "v_vs", "v_part", "v_yb")
    first_local = {k: shapes.pop(k) for k in first}
    later = ("dheld", "acc", "keep", "yx", "gu", "nrm", "sqa", "part", "yb")
    later_local = {k: shapes.pop(k) for k in later}
    anywhere = pl.BlockSpec(memory_space=pl.ANY)
    return pl.pallas_call(
        functools.partial(step_kernel, parts, tuple(shapes), tuple(sems), first_local, later_local),
        out_shape=jax.ShapeDtypeStruct((tokens // m, depth), kind),
        in_specs=[VM] * 6 + [anywhere] * 6,
        out_specs=VM,
        scratch_shapes=[pltpu.VMEM(*v) for v in shapes.values()]
        + [pltpu.SemaphoreType.DMA(v) if v else pltpu.SemaphoreType.DMA for v in sems.values()],
        name="step",
        compiler_params=pltpu.CompilerParams(
            collective_id=0, has_side_effects=True, vmem_limit_bytes=67_000_000
        ),
    )(vit, lengths, vgain, mgain, positions, gain, w_qkv, w_proj, w1, w2, weight, down)


def chunk_count(rows):
    for count in (7, 6, 4, 3, 2):
        if rows % (count * 8) == 0:
            return count
    return 1


def local(
    vit_input,
    image_lengths,
    positions,
    vit_ln_gain,
    w_qkv,
    w_proj,
    merger_ln_gain,
    merger_w1,
    merger_w2,
    norm_gain,
    gate_up_weight,
    down_weight,
):
    width, _, head_cols = w_qkv.shape
    slice_width = norm_gain.shape[0]
    hidden_width = gate_up_weight.shape[2]
    chunks = chunk_count(hidden_width)
    rows = hidden_width // chunks
    return whole_step(
        vit_input,
        image_lengths,
        lane_rows(vit_ln_gain),
        lane_rows(merger_ln_gain),
        lane_rows(positions),
        lane_rows(norm_gain),
        w_qkv.transpose(1, 2, 0).reshape(3 * head_cols, width),
        w_proj,
        merger_w1,
        merger_w2,
        gate_up_weight.transpose(1, 2, 0).reshape(2, chunks, rows, slice_width),
        down_weight.reshape(chunks, rows, slice_width),
    )


def solution(mesh):
    return jax.shard_map(
        local,
        mesh=mesh,
        in_specs=(
            P(("seq", "tp"), None),
            P("seq", None),
            P(),
            P(),
            P(None, None, "tp"),
            P("tp", None),
            P(),
            P(None, "tp"),
            P("tp", None),
            P("seq"),
            P("seq", None, "tp"),
            P("tp", "seq"),
        ),
        out_specs=P("tp", "seq"),
        check_vma=False,
    )
```

```python
import functools

import jax
import jax.numpy as jnp
from jax import lax
from jax.experimental import pallas as pl
from jax.experimental.pallas import tpu as pltpu
from jax.sharding import PartitionSpec as P

HD = 80
MESH = pl.DeviceIdType.MESH
LAG_C, LAG_D, LAG_E = 3, 5, 6
UNITS = 2
AT_PASS, AT_GATHER, AT_RELAY = (0, 1), (2, 3), (2, 3)
VM = pl.BlockSpec(memory_space=pltpu.VMEM)


def factors(n):
    minor = max(d for d in range(1, n + 1) if n % d == 0 and d * d <= n)
    return n // minor, minor


def grid_peers(n_a, n_b, a, b):
    along_a = [lax.rem(a + da, n_a) * n_b + b for da in range(1, n_a)]
    along_b = [a * n_b + lax.rem(b + db, n_b) for db in range(1, n_b)]
    return along_a, along_b


def remote(src, dst, send_sem, recv_sem, axis, peer):
    return pltpu.make_async_remote_copy(
        src_ref=src,
        dst_ref=dst,
        send_sem=send_sem,
        recv_sem=recv_sem,
        device_id={axis: peer},
        device_id_type=MESH,
    )


class LineGather:
    def __init__(self, view, sems):
        n = lax.axis_size("tp")
        self.n_a, self.n_b = factors(n)
        me = lax.axis_index("tp")
        self.a, self.b = me // self.n_b, lax.rem(me, self.n_b)
        self.minors = grid_peers(self.n_a, self.n_b, self.a, self.b)[1]
        self.view, self.sems = view, sems

    def up(self, u, src):
        block = self.view(u, src * self.n_b + self.b)
        send, recv = self.sems["u_s"].at[u, src], self.sems["u_r"].at[u, src]
        return remote(block, block, send, recv, "tp", lax.rem(self.a + 1, self.n_a) * self.n_b + self.b)

    def down(self, u, src):
        block = self.view(u, src * self.n_b + self.b)
        send, recv = self.sems["d_s"].at[u, src], self.sems["d_r"].at[u, src]
        return remote(block, block, send, recv, "tp", lax.rem(self.a + self.n_a - 1, self.n_a) * self.n_b + self.b)

    def minor(self, u, src, db):
        block = self.view(u, src * self.n_b + self.b)
        send, recv = self.sems["m_s"].at[u, src, db - 1], self.sems["m_r"].at[u, src, db - 1]
        return remote(block, block, send, recv, "tp", self.minors[db - 1])

    def send(self, u, src, upward, downward):
        if upward:
            @pl.when(self.a < self.n_a - 1)
            def _():
                self.up(u, src).start()
        if downward:
            @pl.when(self.a > 0)
            def _():
                self.down(u, src).start()
        for db in range(1, self.n_b):
            self.minor(u, src, db).start()

    def start(self, u):
        self.send(u, self.a, True, True)

    def relay(self, u, k):
        @pl.when(self.a >= k)
        def _():
            self.up(u, self.a - k).wait_recv()
            self.send(u, self.a - k, True, False)

        @pl.when(self.a + k < self.n_a)
        def _():
            self.down(u, self.a + k).wait_recv()
            self.send(u, self.a + k, False, True)

    def finish(self, u):
        for src in range(self.n_a):
            for db in range(1, self.n_b):
                self.minor(u, src, db).wait()

            @pl.when(jnp.logical_and(src <= self.a, self.a < self.n_a - 1))
            def _():
                self.up(u, src).wait_send()

            @pl.when(jnp.logical_and(src >= self.a, self.a > 0))
            def _():
                self.down(u, src).wait_send()


def line_sems(units):
    m_a, m_b = factors(lax.axis_size("tp"))
    return {
        "u_s": (units, m_a), "u_r": (units, m_a), "d_s": (units, m_a), "d_r": (units, m_a),
        "m_s": (units, m_a, m_b), "m_r": (units, m_a, m_b),
    }


class ScatterSum:
    def __init__(self, part, r1, yb, r2, sems):
        m = lax.axis_size("tp")
        self.n_a, self.n_b = factors(m)
        me = lax.axis_index("tp")
        self.a, self.b = me // self.n_b, lax.rem(me, self.n_b)
        self.majors, self.minors = grid_peers(self.n_a, self.n_b, self.a, self.b)
        self.part, self.r1, self.yb, self.r2, self.sems = part, r1, yb, r2, sems
        self.order = sorted(range(1, self.n_a), key=lambda da: -min(da, self.n_a - da)) + [0]

    def slot(self, u):
        return lax.rem(u, self.part.shape[0])

    def minor(self, u, da, db):
        at = lax.rem(self.a + da, self.n_a) * self.n_b + lax.rem(self.b + db, self.n_b)
        send, recv = self.sems["rb_s"].at[u, da, db - 1], self.sems["rb_r"].at[u, da, db - 1]
        return remote(self.part.at[self.slot(u), at], self.r1.at[u, da, db - 1], send, recv, "tp", self.minors[db - 1])

    def major(self, u, da):
        send, recv = self.sems["ra_s"].at[u, da - 1], self.sems["ra_r"].at[u, da - 1]
        return remote(self.yb.at[self.slot(u), da - 1], self.r2.at[u, da - 1], send, recv, "tp", self.majors[da - 1])

    def start(self, u):
        for da in self.order:
            for db in range(1, self.n_b):
                self.minor(u, da, db).start()

    def arrived(self, u, da):
        total = self.part[self.slot(u), lax.rem(self.a + da, self.n_a) * self.n_b + self.b].astype(jnp.float32)
        for db in range(1, self.n_b):
            self.minor(u, da, db).wait_recv()
            total = total + self.r1[u, da, db - 1].astype(jnp.float32)
        return total

    def forward(self, u):
        for da in self.order[:-1]:
            self.yb[self.slot(u), da - 1] = self.arrived(u, da).astype(self.yb.dtype)
            self.major(u, da).start()

    def finish(self, u):
        total = self.arrived(u, 0)
        for da in self.order[:-1]:
            self.major(u, da).wait_recv()
            total = total + self.r2[u, da - 1].astype(jnp.float32)
        for da in self.order:
            for db in range(1, self.n_b):
                self.minor(u, da, db).wait_send()
        for da in self.order[:-1]:
            self.major(u, da).wait_send()
        return total


def scatter_sems(units):
    m_a, m_b = factors(lax.axis_size("tp"))
    return {"rb_s": (units, m_a, m_b), "rb_r": (units, m_a, m_b), "ra_s": (units, m_a), "ra_r": (units, m_a)}


def scatter_shapes(units, slots, block, kind):
    m_a, m_b = factors(lax.axis_size("tp"))
    return {
        "part": ((slots, m_a * m_b) + block, kind),
        "r1": ((units, m_a, m_b - 1) + block, kind),
        "yb": ((slots, m_a - 1) + block, kind),
        "r2": ((units, m_a - 1) + block, kind),
    }


def lane_rows(vector):
    return vector.reshape(-1, 128)


def one_row(ref, first=0, count=None):
    count = ref.shape[0] if count is None else count
    return jnp.concatenate([ref[pl.ds(first + k, 1)] for k in range(count)], axis=1)


def normalize(values, gain):
    mean = jnp.mean(values, axis=-1, keepdims=True)
    centered = values - mean
    variance = jnp.mean(centered * centered, axis=-1, keepdims=True)
    return centered * lax.rsqrt(variance + 1e-06) * gain


def keyed(prefix, named):
    return {prefix + k: v for k, v in named.items()}


def under(prefix, named):
    return {k[len(prefix):]: v for k, v in named.items() if k.startswith(prefix)}


def vision_stage(vit_ref, len_ref, gain_ref, gain2_ref, loads, buf, sem, enter, emit):
    m = lax.axis_size("tp")
    m_a, m_b = factors(m)
    mt = lax.axis_index("tp")
    own, width = vit_ref.shape
    half = buf["ag"].shape[-1]
    units = width // half
    heads_wide = buf["wp"].shape[0]
    f32, kind = jnp.float32, vit_ref.dtype
    ag, ag2, vo, part, qkv, att = (buf[k] for k in ("ag", "ag2", "vo", "part", "qkv", "att"))
    first = normalize(vit_ref[...].astype(f32), one_row(gain_ref)).astype(kind)
    for q in range(units):
        ag[q, mt] = first[:, q * half : (q + 1) * half]
    enter()

    def unit_view(u, at):
        return ag.at[u, at]

    gather_one = LineGather(unit_view, sem)
    for u in range(units):
        gather_one.start(u)
    for k in range(1, m_a):
        for u in range(units):
            gather_one.relay(u, k)
    loads["wq"].wait()
    patches = m * own
    for u in range(units):
        gather_one.finish(u)
        piece = lax.dot_general(
            buf["wq"][:, u * half : (u + 1) * half],
            ag[u].reshape(patches, half),
            (((1,), (1,)), ((), ())),
            preferred_element_type=f32,
        )
        if u == 0:
            qkv[...] = piece
        else:
            qkv[...] += piece

    ends = jnp.zeros((1, 1), jnp.int32)
    ids_row = jnp.zeros((1, patches), jnp.int32)
    ids_col = jnp.zeros((patches, 1), jnp.int32)
    at_row = lax.broadcasted_iota(jnp.int32, (1, patches), 1)
    at_col = lax.broadcasted_iota(jnp.int32, (patches, 1), 0)
    for image in range(len_ref.shape[1]):
        ends = ends + len_ref[:, image : image + 1]
        ids_row = ids_row + (at_row >= ends * 4).astype(jnp.int32)
        ids_col = ids_col + (at_col >= ends * 4).astype(jnp.int32)
    same = ids_col == ids_row
    for head in range(heads_wide // HD):
        query, keys, values = (
            qkv[c * heads_wide + head * HD : c * heads_wide + (head + 1) * HD].astype(kind) for c in range(3)
        )
        scores = lax.dot_general(keys, query, (((0,), (0,)), ((), ())), preferred_element_type=f32) * HD ** (-0.5)
        scores = jnp.where(same, scores, -1e30)
        top = jnp.max(scores, axis=0, keepdims=True)
        expo = jnp.exp(scores - top)
        weights = (expo / jnp.sum(expo, axis=0, keepdims=True)).astype(kind)
        att[head * HD : (head + 1) * HD] = jnp.dot(values, weights, preferred_element_type=f32).astype(kind)
    loads["wp"].wait()
    total = ScatterSum(part, buf["r1"], buf["yb"], buf["r2"], sem)
    for u in range(units):
        piece = lax.dot_general(
            att[...], buf["wp"][:, u * half : (u + 1) * half], (((0,), (0,)), ((), ())), preferred_element_type=f32
        )
        part[u] = piece.astype(kind).reshape(m, own, half)
        total.start(u)
    for u in range(units):
        total.forward(u)
    for u in range(units):
        at = slice(u * half, (u + 1) * half)
        vo[:, at] = vit_ref[:, at].astype(f32) + total.finish(u)
    second = normalize(vo[...], one_row(gain2_ref))
    for k in range(width // 128):
        buf["vs"][k] = second[:, k * 128 : (k + 1) * 128]
    tokens = own // 4

    def merged_view(u, at):
        return ag2.at[u - units, :, at]

    gather_two = LineGather(merged_view, sem)
    for q in range(units):
        for j in range(4):
            for k in range(half // 128):
                ag2[q, j, mt, :, k * 128 : (k + 1) * 128] = buf["vs"][
                    q * half // 128 + k, pl.ds(j, tokens, stride=4), :
                ].astype(kind)
        gather_two.start(q + units)
    for k in range(1, m_a):
        for u in range(units):
            gather_two.relay(u + units, k)
    loads["w1"].wait()
    pieces = pieces_of(buf["w1"].shape[1])

    def product(u, piece):
        start, stop = pieces[piece]
        total = None
        for j in range(4):
            at = j * width + u * half
            term = jnp.dot(
                ag2[u, j].reshape(m * tokens, half), buf["w1"][at : at + half, start:stop], preferred_element_type=f32
            )
            total = term if total is None else total + term
        return total

    sums = [0.0, 0.0]
    for u in range(units - 1):
        gather_two.finish(u + units)
        for piece in range(2):
            sums[piece] = sums[piece] + product(u, piece)
    gather_two.finish(2 * units - 1)
    for piece in range(2):
        expanded = sums[piece] + product(units - 1, piece)
        emit(piece, (0.5 * expanded * (1.0 + lax.erf(expanded * 0.5**0.5))).astype(kind))


def pieces_of(width):
    middle = -(-width // 256) * 128
    return [(0, middle), (middle, width)]


def vision_parts(own, width, heads_wide, hidden, kind):
    m, half, f32 = lax.axis_size("tp"), width // 2, jnp.float32
    units = width // half
    shapes = {
        "ag": ((units, m, own, half), kind),
        "wq": ((3 * heads_wide, width), kind),
        "wp": ((heads_wide, width), kind),
        "w1": ((4 * width, hidden), kind),
        "qkv": ((3 * heads_wide, m * own), f32),
        "att": ((heads_wide, m * own), kind),
        "vo": ((own, width), f32),
        "vs": ((width // 128, own, 128), f32),
        "ag2": ((units, 4, m, own // 4, half), kind),
    }
    shapes |= scatter_shapes(units, units, (own, half), kind)
    return shapes, {"wq": (), "wp": (), "w1": ()} | line_sems(2 * units) | scatter_sems(units)


def step_kernel(
    parts, buf_names, sem_names, first_local, later_local, vit_ref, len_ref, vgain_ref, mgain_ref, pos_ref, gain_ref,
    wq_ref, wp_ref, w1_ref, w2_ref, w_ref, d_ref, out_ref, *scratch
):
    buf = dict(zip(buf_names, scratch))
    sem = dict(zip(sem_names, scratch[len(buf_names):]))
    n, m = lax.axis_size("seq"), lax.axis_size("tp")
    (n_a, n_b), (m_a, m_b) = factors(n), factors(m)
    me, mt = lax.axis_index("seq"), lax.axis_index("tp")
    a, b = me // n_b, lax.rem(me, n_b)
    ta, tb = mt // m_b, lax.rem(mt, m_b)
    x_peers, core_peers = grid_peers(n_a, n_b, a, b)
    t_major, t_minor = grid_peers(m_a, m_b, ta, tb)
    partner = core_peers[0]
    chunks, rows, depth = w_ref.shape[1:]
    steps = parts * chunks
    owned = steps // n_b
    count = n_a * 128
    block = count // m
    half = depth // UNITS
    tokens = parts * count
    places = one_row(pos_ref)

    def to(axis, src, dst, s, r, peer):
        return remote(src, dst, s, r, axis, peer)

    def lanes(owner):
        return pl.ds(pl.multiple_of(owner * 128, 128), 128)

    w2_load = pltpu.make_async_copy(
        w2_ref.at[:, pl.ds(pl.multiple_of(me * depth, depth), depth)], buf["w2s"], sem["w2"]
    )

    def w_load(i):
        slot = lax.rem(i, 2)
        return pltpu.make_async_copy(w_ref.at[:, lax.rem(i, chunks)], buf["held"].at[slot], sem["w"].at[slot])

    def d_load(i):
        slot = lax.rem(i, 2)
        return pltpu.make_async_copy(d_ref.at[lax.rem(i, chunks)], buf["dheld"].at[slot], sem["d"].at[slot])


    barrier = pltpu.get_barrier_semaphore()
    everyone = [("seq", lax.rem(me + d, n)) for d in range(1, n)]
    everyone += [("tp", peer) for peer in t_major + t_minor]

    def enter():
        pl.semaphore_wait(barrier, len(everyone))

    ex = buf["ex"]
    columns = [pl.ds(start, stop - start) for start, stop in pieces_of(ex.shape[2])]

    def ex_x(piece, da):
        own = ex.at[me, :, columns[piece]]
        return to("seq", own, own, sem["ea_s"].at[piece, da - 1], sem["ea_r"].at[piece, da - 1], x_peers[da - 1])

    def ex_core(piece, da):
        held = ex.at[lax.rem(a - da + n_a, n_a) * n_b + b, :, columns[piece]]
        return to("seq", held, held, sem["eb_s"].at[piece, da], sem["eb_r"].at[piece, da], partner)

    def emit(piece, values):
        ex[me, :, columns[piece]] = values
        for da in range(1, n_a):
            ex_x(piece, da).start()
        ex_core(piece, 0).start()

    def first_half(**own):
        loads = {
            k: pltpu.make_async_copy(ref, own["v_" + k], sem["v_" + k])
            for k, ref in (("wq", wq_ref), ("wp", wp_ref), ("w1", w1_ref))
        }
        for copy in loads.values():
            copy.start()
        w2_load.start()
        w_load(0).start()
        for axis, peer in everyone:
            pl.semaphore_signal(barrier, inc=1, device_id={axis: peer}, device_id_type=MESH)
        vision_stage(
            vit_ref, len_ref, vgain_ref, mgain_ref, loads, under("v_", buf | own), under("v_", sem), enter, emit
        )

    pl.run_scoped(first_half, **{k: pltpu.VMEM(*v) for k, v in first_local.items()})
    for piece in range(2):
        for da in range(1, n_a):
            ex_x(piece, da).wait_recv()
            ex_core(piece, da).start()
    for piece in range(2):
        for da in range(n_a):
            ex_core(piece, da).wait()
        for da in range(1, n_a):
            ex_x(piece, da).wait_send()

    def second_half(**own):
        buf.update(own)
        part, tok = buf["part"], buf["tok"]
        sums = ScatterSum(part, buf["r1"], buf["yb"], buf["r2"], sem)
        tokens_of = LineGather(lambda u, at: tok.at[u, at], sem)

        def ag_start(u):
            tok[u, mt] = sums.finish(u).astype(tok.dtype)
            tokens_of.start(u)

        rq, inv, sqa, nrm = buf["rq"], buf["inv"], buf["sqa"], buf["nrm"]

        def squares(h, d):
            return to(
                "seq", rq.at[h, me], rq.at[h, me], sem["q_s"].at[h, d - 1], sem["q_r"].at[h, d - 1], lax.rem(me + d, n)
            )

        def ag_finish(h):
            tokens_of.finish(h)
            first = lax.rem(h, UNITS) * half
            gain = one_row(gain_ref, lax.rem(h, UNITS) * (half // 128), half // 128)

            def rows_of(t, carry):
                values = tok[h, t].astype(jnp.float32)
                at = pl.ds(pl.multiple_of(t * block, block), block)
                cols = pl.ds(pl.multiple_of(first, 128), half)
                nrm[at, cols] = (values * gain).astype(nrm.dtype)
                total = values[:, :128] * values[:, :128]
                for k in range(1, half // 128):
                    piece = values[:, k * 128 : (k + 1) * 128]
                    total = total + piece * piece
                sqa[lax.rem(h, UNITS), at] = total
                return carry

            lax.fori_loop(0, m, rows_of, 0)

        def ag_both(h):
            for q in range(UNITS):
                ag_finish(UNITS * h + q)
            squared = jnp.sum(jnp.transpose(jnp.sum(sqa[...], axis=0)), axis=0, keepdims=True)
            rq[h, me] = jnp.broadcast_to(squared, (8, count))
            for d in range(1, n):
                squares(h, d).start()

        def inverse(h):
            for d in range(1, n):
                squares(h, d).wait()
            total = rq[h, 0]
            for s in range(1, n):
                total = total + rq[h, s]
            inv[h] = lax.rsqrt(total / (depth * n) + 1e-06)

        w2_load.wait()
        for h in range(parts):
            row = lax.broadcasted_iota(jnp.int32, (count, tokens), 0)
            slot = lax.shift_right_logical(row, block.bit_length() - 1) * (block * (parts - 1)) + row + h * block
            pick = (slot == places).astype(jnp.bfloat16)
            moved = jnp.dot(
                pick, ex[...].reshape(tokens, ex.shape[2]), preferred_element_type=jnp.float32
            ).astype(jnp.bfloat16)
            width = min(512, half)
            for k in range(depth // width):
                piece = jnp.dot(
                    moved, buf["w2s"][:, k * width : (k + 1) * width], preferred_element_type=jnp.float32
                ).astype(part.dtype)
                q, at = k * width // half, k * width % half
                part[UNITS * h + q, :, :, at : at + width] = piece.reshape(m, block, width)
                if h == 0 and at + width == half:
                    sums.start(q)
        for u in range(UNITS):
            sums.forward(u)
        for t in range(UNITS + m_a - 1):
            if t < UNITS:
                ag_start(t)
            for k in range(1, m_a):
                if 0 <= t - k < UNITS:
                    tokens_of.relay(t - k, k)
        if parts > 1:
            for u in range(UNITS, 2 * UNITS):
                sums.start(u)
        ag_both(0)

        gu, pin, keep, yx, rx, hid, acc = (buf[k] for k in ("gu", "pin", "keep", "yx", "rx", "hid", "acc"))

        def owner(i):
            return lax.rem(i, n_b) == b

        def to_owner(i):
            return to("seq", gu.at[lax.rem(i, 2)], pin.at[i // n_b], sem["p_s"].at[i // n_b], sem["p_r"].at[i // n_b], partner)

        def to_x(i, da):
            o = i // n_b
            return to(
                "seq", yx.at[lax.rem(o, 4), da - 1], rx.at[o, da - 1], sem["y_s"].at[o, da - 1], sem["y_r"].at[o, da - 1], x_peers[da - 1]
            )

        def hid_x(i, da):
            target = hid.at[i, :, lanes(a)]
            return to("seq", target, target, sem["h_s"].at[i, da - 1], sem["h_r"].at[i, da - 1], x_peers[da - 1])

        def hid_core(i, da):
            target = hid.at[i, :, lanes(lax.rem(a - da + n_a, n_a))]
            return to("seq", target, target, sem["o_s"].at[i, da], sem["b_r"].at[i, da], partner)

        def stage_a(i):
            w_load(i).wait()

            @pl.when(i + 1 < steps)
            def _():
                w_load(i + 1).start()

            for half in range(2):
                gu[lax.rem(i, 2), half] = lax.dot_general(
                    buf["held"][lax.rem(i, 2), half],
                    nrm[...],
                    (((1,), (1,)), ((), ())),
                    preferred_element_type=jnp.float32,
                ).astype(gu.dtype)

            @pl.when(jnp.logical_not(owner(i)))
            def _():
                to_owner(i).start()

        def stage_b(i):
            o = i // n_b

            @pl.when(owner(i))
            def _():
                to_owner(i).wait_recv()

                def both(da):
                    at = lanes(lax.rem(a + da, n_a))
                    return gu[lax.rem(i, 2), :, :, at].astype(jnp.float32) + pin[o, :, :, at].astype(jnp.float32)

                for da in range(1, n_a):
                    yx[lax.rem(o, 4), da - 1] = both(da).astype(yx.dtype)
                    to_x(i, da).start()
                keep[lax.rem(o, 2)] = both(0)

            @pl.when(jnp.logical_not(owner(i)))
            def _():
                to_owner(i).wait_send()

        def stage_c(i):
            o, h = i // n_b, i // chunks

            @pl.when(lax.rem(i, chunks) == 0)
            def _():
                inverse(h)

            @pl.when(owner(i))
            def _():
                total = keep[lax.rem(o, 2)]
                for da in range(1, n_a):
                    to_x(i, da).wait()
                    total = total + rx[o, da - 1].astype(jnp.float32)
                total = total * inv[h, 0:1, lanes(a)]
                hid[i, :, lanes(a)] = (jax.nn.silu(total[0]) * total[1]).astype(hid.dtype)
                for da in range(1, n_a):
                    hid_x(i, da).start()
                hid_core(i, 0).start()

        def stage_d(i):
            @pl.when(owner(i))
            def _():
                for da in range(1, n_a):
                    hid_x(i, da).wait()
                    hid_core(i, da).start()

        def stage_e(i):
            c, h = lax.rem(i, chunks), i // chunks

            @pl.when(owner(i))
            def _():
                for da in range(n_a):
                    hid_core(i, da).wait_send()

            @pl.when(jnp.logical_not(owner(i)))
            def _():
                for da in range(n_a):
                    hid_core(i, da).wait_recv()

            d_load(i).wait()
            width = min(512, half)
            left = hid[i]
            for k in range(depth // width):
                at = slice(k * width, (k + 1) * width)
                piece = lax.dot_general(
                    left, buf["dheld"][lax.rem(i, 2), :, at], (((0,), (0,)), ((), ())), preferred_element_type=jnp.float32
                )

                @pl.when(c == 0)
                def _():
                    acc[:, at] = piece

                @pl.when(jnp.logical_and(c > 0, c < chunks - 1))
                def _():
                    acc[:, at] += piece

                @pl.when(c == chunks - 1)
                def _():
                    q, first = k * width // half, k * width % half
                    last = (acc[:, at] + piece).astype(part.dtype)
                    part[UNITS * h + q, :, :, first : first + width] = last.reshape(m, block, width)
                    if first + width == half:
                        sums.start((parts + h) * UNITS + q)

        def down_pass(h):
            for q in range(UNITS):
                sums.forward((parts + h) * UNITS + q)

        def output(h):
            at = pl.ds(pl.multiple_of(h * block, block), block)
            for q in range(UNITS):
                total = sums.finish((parts + h) * UNITS + q)
                out_ref[at, q * half : (q + 1) * half] = (
                    tok[UNITS * h + q, mt].astype(jnp.float32) + total
                ).astype(out_ref.dtype)

        def iteration(i, carry):
            def when(lag, fn):
                @pl.when(jnp.logical_and(i >= lag, i - lag < steps))
                def _():
                    fn(i - lag)

            h, k = i // chunks, lax.rem(i, chunks)
            more = h + 1 < parts

            def at_step(step, q, fn):
                @pl.when(jnp.logical_and(more, k == step * chunks // 7))
                def _():
                    fn(UNITS * (h + 1) + q)

            @pl.when(jnp.logical_and(jnp.logical_and(i > 0, i < steps), k == 0))
            def _():
                @pl.when(more)
                def _():
                    for q in range(UNITS):
                        sums.start(UNITS * (h + 1) + q)

                ag_both(h)

            when(LAG_E - 1, lambda j: d_load(j).start())
            when(0, stage_a)
            when(1, stage_b)
            when(LAG_C, stage_c)
            when(LAG_D, stage_d)
            for q in range(UNITS):
                at_step(AT_PASS[q * 2 // UNITS], q, sums.forward)
            for q in range(UNITS):
                at_step(AT_GATHER[q * 2 // UNITS], q, ag_start)
            for hop in range(1, m_a):
                for q in range(UNITS):
                    at_step(AT_RELAY[q * 2 // UNITS] + hop, q, lambda u, hop=hop: tokens_of.relay(u, hop))
            when(LAG_E, stage_e)

            def later(lag, fn):
                @pl.when(jnp.logical_and(i - lag >= chunks, jnp.logical_and(lax.rem(i - lag + chunks, chunks) == 0, i - lag < steps)))
                def _():
                    fn((i - lag) // chunks - 1)

            later(LAG_E + 1, down_pass)
            later(LAG_E + 3, output)
            return carry

        lax.fori_loop(0, steps + LAG_E, iteration, 0)
        down_pass(parts - 1)
        output(parts - 1)

    pl.run_scoped(second_half, **{k: pltpu.VMEM(*v) for k, v in later_local.items()})


def whole_step(vit, lengths, vgain, mgain, positions, gain, w_qkv, w_proj, w1, w2, weight, down):
    n, m = lax.axis_size("seq"), lax.axis_size("tp")
    (n_a, n_b), (m_a, m_b) = factors(n), factors(m)
    _, chunks, rows, depth = weight.shape
    tokens = positions.size
    count = n_a * 128
    parts = tokens // count
    steps = parts * chunks
    block = count // m
    assert n_b == 2 and steps % 2 == 0 and chunks >= 7
    kind, f32 = vit.dtype, jnp.float32
    own, width = vit.shape
    group = m * own // 4
    shapes = {
        "ex": ((n, group, w1.shape[1]), kind),
        "w2s": ((w2.shape[0], depth), kind),
        "tok": ((UNITS * parts, m, block, depth // UNITS), kind),
        "nrm": ((count, depth), kind),
        "sqa": ((UNITS, count, 128), f32),
        "rq": ((parts, n, 8, count), f32),
        "inv": ((parts, 8, count), f32),
        "held": ((2, 2, rows, depth), kind),
        "dheld": ((2, rows, depth), kind),
        "gu": ((2, 2, rows, count), kind),
        "pin": ((steps // 2, 2, rows, count), kind),
        "keep": ((2, 2, rows, 128), f32),
        "yx": ((4, n_a - 1, 2, rows, 128), kind),
        "rx": ((steps // 2, n_a - 1, 2, rows, 128), kind),
        "hid": ((steps, rows, count), kind),
        "acc": ((count, depth), f32),
    }
    shapes |= scatter_shapes(2 * UNITS * parts, UNITS * parts, (block, depth // UNITS), kind)
    sems = {
        "w2": (),
        "w": (2,),
        "d": (2,),
        "ea_s": (2, n_a),
        "ea_r": (2, n_a),
        "eb_s": (2, n_a),
        "eb_r": (2, n_a),
        "q_s": (parts, n),
        "q_r": (parts, n),
        "p_s": (steps // 2,),
        "p_r": (steps // 2,),
        "y_s": (steps // 2, n_a),
        "y_r": (steps // 2, n_a),
        "h_s": (steps, n_a),
        "h_r": (steps, n_a),
        "o_s": (steps, n_a),
        "b_r": (steps, n_a),
    }
    sems |= scatter_sems(2 * UNITS * parts) | line_sems(UNITS * parts)
    v_shapes, v_sems = vision_parts(own, width, w_proj.shape[0], w1.shape[1], kind)
    shapes |= keyed("v_", v_shapes)
    sems |= keyed("v_", v_sems)
    first = ("v_wq", "v_wp", "v_w1", "v_qkv", "v_att", "v_vo", "v_vs", "v_part", "v_yb")
    first_local = {k: shapes.pop(k) for k in first}
    later = ("dheld", "acc", "keep", "yx", "gu", "nrm", "sqa", "part", "yb")
    later_local = {k: shapes.pop(k) for k in later}
    anywhere = pl.BlockSpec(memory_space=pl.ANY)
    return pl.pallas_call(
        functools.partial(step_kernel, parts, tuple(shapes), tuple(sems), first_local, later_local),
        out_shape=jax.ShapeDtypeStruct((tokens // m, depth), kind),
        in_specs=[VM] * 6 + [anywhere] * 6,
        out_specs=VM,
        scratch_shapes=[pltpu.VMEM(*v) for v in shapes.values()]
        + [pltpu.SemaphoreType.DMA(v) if v else pltpu.SemaphoreType.DMA for v in sems.values()],
        name="step",
        compiler_params=pltpu.CompilerParams(
            collective_id=0, has_side_effects=True, vmem_limit_bytes=67_000_000
        ),
    )(vit, lengths, vgain, mgain, positions, gain, w_qkv, w_proj, w1, w2, weight, down)


def chunk_count(rows):
    for count in (7, 6, 4, 3, 2):
        if rows % (count * 8) == 0:
            return count
    return 1


def local(
    vit_input,
    image_lengths,
    positions,
    vit_ln_gain,
    w_qkv,
    w_proj,
    merger_ln_gain,
    merger_w1,
    merger_w2,
    norm_gain,
    gate_up_weight,
    down_weight,
):
    width, _, head_cols = w_qkv.shape
    slice_width = norm_gain.shape[0]
    hidden_width = gate_up_weight.shape[2]
    chunks = chunk_count(hidden_width)
    rows = hidden_width // chunks
    return whole_step(
        vit_input,
        image_lengths,
        lane_rows(vit_ln_gain),
        lane_rows(merger_ln_gain),
        lane_rows(positions),
        lane_rows(norm_gain),
        w_qkv.transpose(1, 2, 0).reshape(3 * head_cols, width),
        w_proj,
        merger_w1,
        merger_w2,
        gate_up_weight.transpose(1, 2, 0).reshape(2, chunks, rows, slice_width),
        down_weight.reshape(chunks, rows, slice_width),
    )


def solution(mesh):
    return jax.shard_map(
        local,
        mesh=mesh,
        in_specs=(
            P(("seq", "tp"), None),
            P("seq", None),
            P(),
            P(),
            P(None, None, "tp"),
            P("tp", None),
            P(),
            P(None, "tp"),
            P("tp", None),
            P("seq"),
            P("seq", None, "tp"),
            P("tp", "seq"),
        ),
        out_specs=P("tp", "seq"),
        check_vma=False,
    )
```
